512 devices in a mesh: dap: 32 (over x_lo, z, core), ch: 16 (over y, x_hi).
Axes of the slice: x: 4 (x_hi: 2, x_lo: 2; x = x_hi * 2 + x_lo), y: 8, z: 8, core: 2. Of those that a mesh axis runs over, the one named last changes fastest.
Arguments:
- pair_rep: bfloat16 [480, 480, 128], P('dap', 'ch'), may hold values from -400 to 400
- residue_mask: int32 [480], replicated, may hold values 0 or 1
- w_proj: bfloat16 [128, 512], replicated, may hold values from -0.5 to 0.5
- w_gate: bfloat16 [128, 128], replicated, may hold values from -0.5 to 0.5
- w_out: bfloat16 [128, 128], replicated, may hold values from -0.5 to 0.5
- cotangent: bfloat16 [480, 480, 128], P('dap', 'ch'), may hold values from -6 to 6
Outputs:
- pair_update: bfloat16 [480, 480, 128], P('dap', 'ch')
- grad_pair: bfloat16 [480, 480, 128], P('dap', 'ch')
The draws below stay inside these ranges and needn't reach their ends.
Inputs may be any that keep to these rules, and one draw needn't show every extreme that they name: `residue_mask`: 1 marks a residue of the crop, 0 a padding position.
All inputs are finite; a program needn't handle non-finite values.
Results may differ from the reference program's by a relative error of at most 0.0085.
Values may be sent and summed in bfloat16 or wider, within the bound.
A program may use at most 64 MiB of HBM per device.

```python
import math
import jax
import jax.numpy as jnp
from jax import lax

C = 128
H = 128
N_RES = 480


def draw_pair_rep(key, part):
    subkeys = jax.random.split(jax.random.fold_in(key, 11), 4)
    full_shape = (N_RES, N_RES, C)
    channel_scale = jnp.exp(jax.random.uniform(subkeys[2], (1, 1, C), jnp.float32, 0.0, math.log(4.0)))
    cell_offset = 0.5 * jnp.clip(jax.random.normal(subkeys[3], (N_RES, N_RES, 1), jnp.float32), -4.0, 4.0)
    cell_scale = jnp.exp(jax.random.uniform(subkeys[1], (N_RES, N_RES, 1), jnp.float32, 0.0, math.log(10.0)))
    base_values = jnp.clip(jax.random.normal(subkeys[0], full_shape, jnp.float32), -4.0, 4.0) + cell_offset
    return (base_values * cell_scale * channel_scale).astype(jnp.bfloat16)


def touch_ends(result, key, least, largest):
    longest = result.shape.index(max(result.shape))
    spots = []
    for shift in (0, 1):
        where = [jax.random.randint(jax.random.fold_in(key, axis), (), 0, length) for axis, length in enumerate(result.shape)]
        where[longest] = (where[longest] + shift) % result.shape[longest]
        spots.append(tuple(where))
    return result.at[spots[0]].set(least).at[spots[1]].set(largest)


def level_of(key, extent, shards, least, largest):
    factor_of = 1.0
    for position, shards_of in shards:
        draws = jax.random.uniform(jax.random.fold_in(jax.random.fold_in(key, 6), position), (shards_of,), jnp.float32, least / len(shards), largest / len(shards))
        factor_of = factor_of * jnp.repeat(jnp.exp(draws), extent[position] // shards_of).reshape((-1,) + (1,) * (len(extent) - 1 - position))
    return factor_of


def normal_values(rng, shape, scale, bound, cuts=(), dtype=jnp.bfloat16):
    factor_of = level_of(rng, shape, cuts, -0.22, 0.18) if cuts else 1.0
    values = jax.random.normal(rng, shape, jnp.float32) * scale * factor_of
    return jnp.minimum(jnp.maximum(values, -bound), bound).astype(dtype)


def setup_inputs(seed: int = 0) -> dict:
    key_list = jax.random.split(jax.random.key(seed), 7)
    pair_rep = draw_pair_rep(jax.random.fold_in(key_list[6], 71), 0)
    residue_mask = touch_ends((jax.random.randint(key_list[1], (N_RES,), 0, 8) < 7).astype(jnp.int32), jax.random.fold_in(key_list[1], 1), 0, 1)
    w_proj = normal_values(key_list[2], (C, 4 * H), C ** -0.5, 0.5)
    w_gate = normal_values(key_list[3], (C, C), C ** -0.5, 0.5)
    w_out = normal_values(key_list[4], (H, C), H ** -0.5, 0.5)
    cotangent = normal_values(key_list[5], (N_RES, N_RES, C), 1.0, 6.0, ((0, 32), (1, 16)))
    return dict(pair_rep=pair_rep, residue_mask=residue_mask, w_proj=w_proj, w_gate=w_gate, w_out=w_out, cotangent=cotangent)


EPSILON = 1e-05

def normalize(values, axis):
    center = lax.optimization_barrier(jnp.mean(values, axis=axis, keepdims=True))
    spread = values - center
    scale_inv = lax.rsqrt(lax.optimization_barrier(jnp.mean(spread * spread, axis=axis, keepdims=True)) + EPSILON)
    return (spread * scale_inv, scale_inv)

def norm_back(grad_in, normed, scale_inv, axis):
    first = lax.optimization_barrier(jnp.mean(grad_in, axis=axis, keepdims=True))
    second = lax.optimization_barrier(jnp.mean(grad_in * normed, axis=axis, keepdims=True))
    return scale_inv * (grad_in - first - normed * second)

def reference(pair_rep, residue_mask, w_proj, w_gate, w_out, cotangent):
    live_flags = residue_mask.astype(jnp.float32)
    pair_mask = (live_flags[:, None] * live_flags[None, :])[:, :, None]
    normed, pair_scale = normalize(pair_rep.astype(jnp.float32), 2)
    normed_half = normed.astype(jnp.bfloat16)
    flat_cells = normed_half.reshape(N_RES * N_RES, C)
    projected = jnp.dot(flat_cells, w_proj, preferred_element_type=jnp.float32).reshape(N_RES, N_RES, 4 * H)
    left_sig = jax.nn.sigmoid(projected[:, :, :H])
    left_val = projected[:, :, H:2 * H]
    right_sig = jax.nn.sigmoid(projected[:, :, 2 * H:3 * H])
    right_val = projected[:, :, 3 * H:]
    left_edges = (left_sig * left_val * pair_mask).astype(jnp.bfloat16)
    right_edges = (right_sig * right_val * pair_mask).astype(jnp.bfloat16)
    gate_values = jax.nn.sigmoid(jnp.dot(flat_cells, w_gate, preferred_element_type=jnp.float32).reshape(N_RES, N_RES, C))
    product = jnp.einsum('ikc,jkc->ijc', left_edges.astype(jnp.float32), right_edges.astype(jnp.float32)).astype(jnp.bfloat16)
    hidden_norm, hidden_scale = normalize(product.astype(jnp.float32), 2)
    hidden_half = hidden_norm.astype(jnp.bfloat16)
    projected_out = jnp.dot(hidden_half.reshape(N_RES * N_RES, H), w_out, preferred_element_type=jnp.float32).reshape(N_RES, N_RES, C)
    pair_update = (gate_values * projected_out).astype(jnp.bfloat16)
    upstream = cotangent.astype(jnp.float32)
    grad_out = (upstream * gate_values).astype(jnp.bfloat16)
    grad_logit = (upstream * projected_out * gate_values * (1.0 - gate_values)).astype(jnp.bfloat16)
    grad_hidden = jnp.dot(grad_out.reshape(N_RES * N_RES, C), w_out.T, preferred_element_type=jnp.float32).reshape(N_RES, N_RES, H)
    grad_product = norm_back(grad_hidden, hidden_norm, hidden_scale, 2).astype(jnp.bfloat16)
    grad_left = jnp.einsum('ijc,jkc->ikc', grad_product.astype(jnp.float32), right_edges.astype(jnp.float32)).astype(jnp.bfloat16)
    grad_right = jnp.einsum('ijc,ikc->jkc', grad_product.astype(jnp.float32), left_edges.astype(jnp.float32)).astype(jnp.bfloat16)
    masked_left = grad_left.astype(jnp.float32) * pair_mask
    masked_right = grad_right.astype(jnp.float32) * pair_mask
    grad_proj = jnp.concatenate([masked_left * left_val * left_sig * (1.0 - left_sig), masked_left * left_sig, masked_right * right_val * right_sig * (1.0 - right_sig), masked_right * right_sig], axis=2).astype(jnp.bfloat16)
    grad_normed = jnp.dot(grad_proj.reshape(N_RES * N_RES, 4 * H), w_proj.T, preferred_element_type=jnp.float32)
    grad_normed = grad_normed + jnp.dot(grad_logit.reshape(N_RES * N_RES, C), w_gate.T, preferred_element_type=jnp.float32)
    grad_pair = norm_back(grad_normed.reshape(N_RES, N_RES, C), normed, pair_scale, 2).astype(jnp.bfloat16)
    return (pair_update, grad_pair)
```

```python
import functools

import jax
import jax.numpy as jnp
from jax import lax
from jax.experimental import pallas as pl
from jax.experimental.pallas import tpu as pltpu
from jax.sharding import PartitionSpec as P

EPSILON = 1e-05
F32 = jnp.float32
BF16 = jnp.bfloat16
GROUP = 8
CELLS = 512


def owner_of(channel, dap_size):
    if dap_size == 32:
        return lax.rem(channel, 2) * 16 + 2 * channel + 1
    return channel


def owned_by(me, dap_size):
    if dap_size == 32:
        z = lax.rem(me // 2, 8)
        return z, jnp.logical_and(lax.rem(me, 2) == 1, me // 16 == lax.rem(z, 2))
    return me, me < GROUP


def dot(a, b, contract):
    return lax.dot_general(a, b, (contract, ((), ())), preferred_element_type=F32)


def swap_blocks(rows):
    block = lax.broadcasted_iota(jnp.int32, rows[0].shape, 1) // 32
    odd = lax.rem(block, 2) == 1
    high = block >= 2
    x0, x1, x2, x3 = rows
    z0 = jnp.where(odd, pltpu.roll(x1, 32, 1), x0)
    z1 = jnp.where(odd, x1, pltpu.roll(x0, 96, 1))
    z2 = jnp.where(odd, pltpu.roll(x3, 32, 1), x2)
    z3 = jnp.where(odd, x3, pltpu.roll(x2, 96, 1))
    return (
        jnp.where(high, pltpu.roll(z2, 64, 1), z0),
        jnp.where(high, pltpu.roll(z3, 64, 1), z1),
        jnp.where(high, z2, pltpu.roll(z0, 64, 1)),
        jnp.where(high, z3, pltpu.roll(z1, 64, 1)),
    )


def cells_to_rows(cells, mid, rows):
    for t in range(cells.shape[0] // 4):
        for q in range(4):
            lanes = pl.ds(q * 128, 128)
            moved = swap_blocks([cells[4 * t + a, :, lanes].astype(F32) for a in range(4)])
            for b in range(4):
                mid[t, pl.ds(4 * q + b, GROUP, stride=16), :] = moved[b]
    for t in range(cells.shape[0] // 4):
        for m in range(GROUP):
            rows[m, :, pl.ds(t * 128, 128)] = mid[t, pl.ds(16 * m, 16), :].astype(BF16)


def rows_to_cells(rows, mid, cells):
    for t in range(cells.shape[0] // 4):
        for m in range(GROUP):
            mid[t, pl.ds(16 * m, 16), :] = rows[m, :, pl.ds(t * 128, 128)].astype(F32)
    for t in range(cells.shape[0] // 4):
        for q in range(4):
            lanes = pl.ds(q * 128, 128)
            moved = swap_blocks([mid[t, pl.ds(4 * q + b, GROUP, stride=16), :] for b in range(4)])
            for a in range(4):
                cells[4 * t + a, :, lanes] = moved[a].astype(BF16)


def kernel(
    nd,
    ns,
    x_ref,
    cot_ref,
    mask_ref,
    wp_ref,
    wg_ref,
    wo_ref,
    upd_ref,
    gpair_ref,
    padded,
    live,
    proj,
    normed,
    gate,
    cot,
    ghid,
    glogit,
    mid,
    out1,
    in1,
    out2,
    in2,
    own_in,
    own_out,
    send_sem,
    recv_sem,
):
    rows, columns, chans = x_ref.shape
    half = columns // 2
    hidden = ns * GROUP
    me_d = lax.axis_index("dap")
    me_s = lax.axis_index("ch")
    my_m, is_owner = owned_by(me_d, nd)

    barrier = pltpu.get_barrier_semaphore()

    def greet(peer):
        pl.semaphore_signal(
            barrier, inc=1, device_id=peer, device_id_type=pl.DeviceIdType.MESH
        )

    @pl.loop(1, ns)
    def _(r):
        greet({"ch": lax.rem(me_s + r, ns)})

    @pl.when(is_owner)
    def _():
        @pl.loop(1, nd)
        def _(r):
            greet({"dap": lax.rem(me_d + r, nd)})

    @pl.when(jnp.logical_not(is_owner))
    def _():
        @pl.loop(0, GROUP)
        def _(m):
            greet({"dap": owner_of(m, nd)})

    def push(src, dst, sem, peer):
        return pltpu.make_async_remote_copy(
            src_ref=src,
            dst_ref=dst,
            send_sem=send_sem.at[sem],
            recv_sem=recv_sem.at[sem],
            device_id=peer,
            device_id_type=pl.DeviceIdType.MESH,
        )

    def across_ch(src, dst, sem):
        @pl.loop(1, ns)
        def _(r):
            peer = lax.rem(me_s + r, ns)
            push(src.at[peer], dst.at[me_s], sem, {"ch": peer}).start()

        dst[me_s] = src[me_s]

    def await_ch(dst, sem):
        some = dst.at[pl.ds(0, ns - 1)]
        push(some, some, sem, {"ch": me_s}).wait_recv()

    def to_owners(src, dst, sem):
        @pl.loop(0, GROUP)
        def _(r):
            m = lax.rem(my_m + r, GROUP)
            owner = owner_of(m, nd)

            @pl.when(owner != me_d)
            def _():
                push(src.at[m], dst.at[me_d], sem, {"dap": owner}).start()

            @pl.when(owner == me_d)
            def _():
                dst[me_d] = src[m]

    def await_owner(dst, sem):
        some = dst.at[pl.ds(0, nd - 1)]
        push(some, some, sem, {"dap": me_d}).wait_recv()

    def from_owner(src, dst, sem, d):
        @pl.when(d != me_d)
        def _():
            push(src.at[d], dst.at[my_m], sem, {"dap": d}).start()

        @pl.when(d == me_d)
        def _():
            dst[my_m] = src[d]

    def await_rows(dst, sem):
        @pl.when(is_owner)
        def _():
            some = dst.at[pl.ds(0, GROUP - 1)]
            push(some, some, sem, {"dap": me_d}).wait_recv()

        @pl.when(jnp.logical_not(is_owner))
        def _():
            push(dst, dst, sem, {"dap": me_d}).wait_recv()

    lane = lax.broadcasted_iota(jnp.int32, (1, CELLS), 1)
    place = lax.rem(lane, 16)
    used = jnp.logical_and(place < half, lane < rows * 32)
    first_half = lax.rem(lane, 32) < 16

    eye = (
        lax.broadcasted_iota(jnp.int32, (chans, chans), 0)
        == lax.broadcasted_iota(jnp.int32, (chans, chans), 1)
    ).astype(F32).astype(BF16)

    def cells_first(ref, slot):
        padded[slot] = jnp.zeros(padded.shape[1:], BF16)
        padded[slot, 0:rows, 0:columns, :] = ref[...]
        flat = padded[slot].reshape(CELLS, chans)
        turned = dot(eye, flat, ((1,), (1,)))
        spread = jnp.where(first_half, turned, pltpu.roll(turned, 1, 1))
        return jnp.where(used, spread, 0.0)

    def cells_last(turned):
        closed = jnp.where(
            lax.rem(lane, 32) < half, turned, pltpu.roll(turned, CELLS - 1, 1)
        )
        return closed.T.reshape(16, 32, chans)[0:rows, 0:columns, :].astype(BF16)

    xt = cells_first(x_ref, 0)
    center = jnp.mean(xt, axis=0, keepdims=True)
    spread = xt - center
    pair_scale = lax.rsqrt(jnp.mean(spread * spread, axis=0, keepdims=True) + EPSILON)
    nt = spread * pair_scale
    normed[...] = nt
    nh = nt.astype(BF16)

    residues = mask_ref.shape[1]
    total = nd * 16
    live[...] = jnp.zeros(live.shape, F32)
    live[:, 0:residues] = jnp.broadcast_to(mask_ref[...].astype(F32), (8, residues))
    flags = live[...].astype(BF16)

    def one_hot(hot):
        return jnp.where(hot, 1.0, 0.0).astype(BF16)

    at = lax.broadcasted_iota(jnp.int32, (total, 128), 0)
    lane_1 = lax.broadcasted_iota(jnp.int32, (total, 128), 1)
    row_flags = dot(
        flags, one_hot(jnp.logical_and(at == rows * me_d + lane_1, lane_1 < rows)), ((1,), (0,))
    )
    col_at = columns * me_s + half * (lax.rem(lane_1, 32) // 16) + lax.rem(lane_1, 16)
    col_flags = dot(
        flags, one_hot(jnp.logical_and(at == col_at, lax.rem(lane_1, 16) < half)), ((1,), (0,))
    )
    spot = lax.broadcasted_iota(jnp.int32, (128, CELLS), 0)
    row_of = lax.broadcasted_iota(jnp.int32, (128, CELLS), 1) // 32
    row_mask = dot(row_flags.astype(BF16), one_hot(spot == row_of), ((1,), (0,)))
    col_mask = jnp.concatenate([col_flags] * (CELLS // 128), axis=1)
    mask = (row_mask * col_mask)[0:1]

    def project(part):
        raw = dot(wp_ref[:, pl.ds(part * hidden, hidden)], nh, ((0,), (0,)))
        return raw

    def edge(part, slot):
        sig = jax.nn.sigmoid(project(part))
        val = project(part + 1)
        proj[part] = sig
        proj[part + 1] = val
        out1[slot] = (sig * val * mask).reshape(ns, GROUP, CELLS).astype(BF16)

    edge(0, 0)
    pl.semaphore_wait(barrier, ns - 1 + jnp.where(is_owner, nd - 1, GROUP))
    across_ch(out1.at[0], in1.at[0], 0)
    edge(2, 1)
    across_ch(out1.at[1], in1.at[1], 1)

    gv = jax.nn.sigmoid(dot(wg_ref[...], nh, ((0,), (0,))))
    gate[...] = gv
    ct = cells_first(cot_ref, 1)
    cot[...] = ct
    gh = dot(wo_ref[...], (ct * gv).astype(BF16), ((1,), (0,)))
    ghid[...] = gh - jnp.mean(gh, axis=0, keepdims=True)

    for a in range(2):
        await_ch(in1.at[a], a)
        cells_to_rows(in1.at[a], mid, out2.at[a])
        to_owners(out2.at[a], own_in.at[a], 2 + a)

    width = ns * 32
    per = 128 // 16

    def all_rows(ref):
        return ref[...].reshape(nd * 16, width)

    def return_rows(buffer, back, sem, b, value):
        own_out[buffer, pl.ds(per * b, per)] = value.astype(BF16).reshape(per, 16, width)

        @pl.loop(0, per)
        def _(e):
            from_owner(own_out.at[buffer], in2.at[back], sem, per * b + e)

    @pl.when(is_owner)
    def _():
        await_owner(own_in.at[0], 2)
        await_owner(own_in.at[1], 3)

        @pl.loop(0, nd // per)
        def _(b):
            left = own_in[0, pl.ds(per * b, per)].reshape(128, width)
            return_rows(0, 0, 4, b, dot(left, all_rows(own_in.at[1]), ((1,), (1,))))

    await_rows(in2.at[0], 4)
    rows_to_cells(in2.at[0], mid, out1.at[2])
    across_ch(out1.at[2], in1.at[2], 5)
    await_ch(in1.at[2], 5)

    prod = in1[2].reshape(hidden, CELLS).astype(F32)
    away = prod - jnp.mean(prod, axis=0, keepdims=True)
    hidden_scale = lax.rsqrt(jnp.mean(away * away, axis=0, keepdims=True) + EPSILON)
    hn = away * hidden_scale
    gh_away = ghid[...]
    second = jnp.mean((gh_away) * hn, axis=0, keepdims=True)
    gprod = hidden_scale * (gh_away - hn * second)
    out1[3] = gprod.reshape(ns, GROUP, CELLS).astype(BF16)
    across_ch(out1.at[3], in1.at[3], 6)

    po = dot(wo_ref[...], hn.astype(BF16), ((0,), (0,)))
    gv = gate[...]
    glogit[...] = (cot[...] * po * gv * (1.0 - gv)).astype(BF16)
    upd_ref[...] = cells_last(gv * po)

    await_ch(in1.at[3], 6)
    cells_to_rows(in1.at[3], mid, out2.at[2])
    to_owners(out2.at[2], own_in.at[2], 7)

    @pl.when(is_owner)
    def _():
        await_owner(own_in.at[2], 7)

        @pl.loop(0, nd // per)
        def _(b):
            part = own_in[2, pl.ds(per * b, per)].reshape(128, width)
            return_rows(1, 1, 8, b, dot(part, all_rows(own_in.at[1]), ((1,), (0,))))

        @pl.loop(0, nd // per)
        def _(b):
            lanes = pl.ds(pl.multiple_of(b * 128, 128), 128)
            part = own_in[2, :, :, lanes].reshape(nd * 16, 128)
            return_rows(2, 2, 9, b, dot(part, all_rows(own_in.at[0]), ((0,), (0,))))

    base = dot(wg_ref[...], glogit[...], ((1,), (0,)))

    for a in range(2):
        await_rows(in2.at[1 + a], 8 + a)
        rows_to_cells(in2.at[1 + a], mid, out1.at[4 + a])
        across_ch(out1.at[4 + a], in1.at[4 + a], 10 + a)

    for a in range(2):
        await_ch(in1.at[4 + a], 10 + a)
        masked = in1[4 + a].reshape(hidden, CELLS).astype(F32) * mask
        sig = proj[2 * a]
        val = proj[2 * a + 1]
        to_sig = (masked * val * sig * (1.0 - sig)).astype(BF16)
        to_val = (masked * sig).astype(BF16)
        base = base + dot(wp_ref[:, pl.ds(2 * a * hidden, hidden)], to_sig, ((1,), (0,)))
        base = base + dot(wp_ref[:, pl.ds((2 * a + 1) * hidden, hidden)], to_val, ((1,), (0,)))

    nt = normed[...]
    first = jnp.mean(base, axis=0, keepdims=True)
    second = jnp.mean(base * nt, axis=0, keepdims=True)
    gpair_ref[...] = cells_last(pair_scale * (base - first - nt * second))

    def sent(ref, sem):
        push(ref, ref, sem, {"ch": me_s}).wait_send()

    few = pl.ds(0, ns - 1)
    for buffer, sem in ((0, 0), (1, 1), (2, 5), (3, 6), (4, 10), (5, 11)):
        sent(out1.at[buffer, few], sem)
    for buffer, sem in ((0, 2), (1, 3), (2, 7)):

        @pl.when(is_owner)
        def _():
            sent(out2.at[buffer, pl.ds(0, GROUP - 1)], sem)

        @pl.when(jnp.logical_not(is_owner))
        def _():
            sent(out2.at[buffer], sem)

    @pl.when(is_owner)
    def _():
        for buffer, sem in ((0, 4), (1, 8), (2, 9)):
            sent(own_out.at[buffer, pl.ds(0, nd - 1)], sem)


def on_device(nd, ns, pair_rep, residue_mask, w_proj, w_gate, w_out, cotangent):
    hidden, chans = w_out.shape
    vmem = pl.BlockSpec(memory_space=pltpu.VMEM)
    shape = jax.ShapeDtypeStruct(pair_rep.shape, BF16)
    width = ns * 32
    return pl.pallas_call(
        functools.partial(kernel, nd, ns),
        out_shape=(shape, shape),
        in_specs=[vmem] * 6,
        out_specs=(vmem, vmem),
        scratch_shapes=[
            pltpu.VMEM((2, 16, 32, chans), BF16),
            pltpu.VMEM((8, nd * 16), F32),
            pltpu.VMEM((4, hidden, CELLS), F32),
            pltpu.VMEM((chans, CELLS), F32),
            pltpu.VMEM((chans, CELLS), F32),
            pltpu.VMEM((chans, CELLS), F32),
            pltpu.VMEM((hidden, CELLS), F32),
            pltpu.VMEM((chans, CELLS), BF16),
            pltpu.VMEM((ns // 4, 16 * GROUP, 128), F32),
            pltpu.VMEM((6, ns, GROUP, CELLS), BF16),
            pltpu.VMEM((6, ns, GROUP, CELLS), BF16),
            pltpu.VMEM((3, GROUP, 16, width), BF16),
            pltpu.VMEM((3, GROUP, 16, width), BF16),
            pltpu.VMEM((3, nd, 16, width), BF16),
            pltpu.VMEM((3, nd, 16, width), BF16),
            pltpu.SemaphoreType.DMA((12,)),
            pltpu.SemaphoreType.DMA((12,)),
        ],
        compiler_params=pltpu.CompilerParams(
            collective_id=0, has_side_effects=True, vmem_limit_bytes=48 * 1024 * 1024
        ),
    )(pair_rep, cotangent, residue_mask[None, :], w_proj, w_gate, w_out)


def solution(mesh):
    nd, ns = mesh.shape["dap"], mesh.shape["ch"]
    return jax.shard_map(
        functools.partial(on_device, nd, ns),
        mesh=mesh,
        in_specs=(P("dap", "ch", None), P(), P(), P(), P(), P("dap", "ch", None)),
        out_specs=(P("dap", "ch", None), P("dap", "ch", None)),
        check_vma=False,
    )
```

```python
import functools

import jax
import jax.numpy as jnp
from jax import lax
from jax.experimental import pallas as pl
from jax.experimental.pallas import tpu as pltpu
from jax.sharding import PartitionSpec as P

EPSILON = 1e-05
F32 = jnp.float32
BF16 = jnp.bfloat16
GROUP = 8
CELLS = 512


def owner_of(channel, dap_size):
    if dap_size == 32:
        return lax.rem(channel, 2) * 16 + 2 * channel + 1
    return channel


def owned_by(me, dap_size):
    if dap_size == 32:
        z = lax.rem(me // 2, 8)
        return z, jnp.logical_and(lax.rem(me, 2) == 1, me // 16 == lax.rem(z, 2))
    return me, me < GROUP


def ring_order(size):
    return sorted(range(size), key=lambda r: -min(r, size - r))


def ch_peers(me, ch_size):
    ny = ch_size // 2
    steps = [(dy, dx) for dy in range(ny) for dx in range(2) if dy or dx]
    steps.sort(key=lambda p: -(min(p[0], ny - p[0]) + 2 * p[1]))
    y, x = me // 2, lax.rem(me, 2)
    return [2 * lax.rem(y + dy, ny) + lax.rem(x + dx, 2) for dy, dx in steps]


def dap_peers(me, dap_size):
    if dap_size != 32:
        return [lax.rem(me + r, dap_size) for r in range(1, dap_size)]
    x, z = me // 16, lax.rem(me // 2, 8)
    return [
        16 * lax.rem(x + dx, 2) + 2 * lax.rem(z + dz, 8) + core
        for dz in ring_order(8)
        for dx in (1, 0)
        for core in (0, 1)
        if dz or dx or not core
    ]


def dot(a, b, contract):
    return lax.dot_general(a, b, (contract, ((), ())), preferred_element_type=F32)


def swap_blocks(rows):
    block = lax.broadcasted_iota(jnp.int32, rows[0].shape, 1) // 32
    odd = lax.rem(block, 2) == 1
    high = block >= 2
    x0, x1, x2, x3 = rows
    z0 = jnp.where(odd, pltpu.roll(x1, 32, 1), x0)
    z1 = jnp.where(odd, x1, pltpu.roll(x0, 96, 1))
    z2 = jnp.where(odd, pltpu.roll(x3, 32, 1), x2)
    z3 = jnp.where(odd, x3, pltpu.roll(x2, 96, 1))
    return (
        jnp.where(high, pltpu.roll(z2, 64, 1), z0),
        jnp.where(high, pltpu.roll(z3, 64, 1), z1),
        jnp.where(high, z2, pltpu.roll(z0, 64, 1)),
        jnp.where(high, z3, pltpu.roll(z1, 64, 1)),
    )


def cells_to_rows(cells, mid, rows):
    for t in range(cells.shape[0] // 4):
        for q in range(4):
            lanes = pl.ds(q * 128, 128)
            moved = swap_blocks([cells[4 * t + a, :, lanes].astype(F32) for a in range(4)])
            for b in range(4):
                mid[t, pl.ds(4 * q + b, GROUP, stride=16), :] = moved[b]
    for t in range(cells.shape[0] // 4):
        for m in range(GROUP):
            rows[m, :, pl.ds(t * 128, 128)] = mid[t, pl.ds(16 * m, 16), :].astype(BF16)


def rows_to_cells(rows, mid, cells):
    for t in range(cells.shape[0] // 4):
        for m in range(GROUP):
            mid[t, pl.ds(16 * m, 16), :] = rows[m, :, pl.ds(t * 128, 128)].astype(F32)
    for t in range(cells.shape[0] // 4):
        for q in range(4):
            lanes = pl.ds(q * 128, 128)
            moved = swap_blocks([mid[t, pl.ds(4 * q + b, GROUP, stride=16), :] for b in range(4)])
            for a in range(4):
                cells[4 * t + a, :, lanes] = moved[a].astype(BF16)


def kernel(
    nd,
    ns,
    x_hbm,
    cot_hbm,
    mask_hbm,
    wp_hbm,
    wg_hbm,
    wo_hbm,
    upd_ref,
    gpair_ref,
    x_ref,
    cot_ref,
    mask_ref,
    wp_ref,
    wg_ref,
    wo_ref,
    padded,
    live,
    proj,
    normed,
    gate,
    cot,
    ghid,
    glogit,
    mid,
    out1,
    in1,
    out2,
    in2,
    own_in,
    own_out,
    load_sem,
    send_sem,
    recv_sem,
):
    rows, columns, chans = x_ref.shape
    half = columns // 2
    hidden = ns * GROUP
    me_d = lax.axis_index("dap")
    me_s = lax.axis_index("ch")
    my_m, is_owner = owned_by(me_d, nd)

    loads = [
        pltpu.make_async_copy(src, dst, load_sem.at[n])
        for n, (src, dst) in enumerate(
            (
                (x_hbm, x_ref),
                (wp_hbm, wp_ref),
                (mask_hbm, mask_ref),
                (cot_hbm, cot_ref),
                (wg_hbm, wg_ref),
                (wo_hbm, wo_ref),
            )
        )
    ]
    for load in loads:
        load.start()

    barrier = pltpu.get_barrier_semaphore()

    def greet(peer):
        pl.semaphore_signal(
            barrier, inc=1, device_id=peer, device_id_type=pl.DeviceIdType.MESH
        )

    for peer in ch_peers(me_s, ns):
        greet({"ch": peer})

    @pl.when(is_owner)
    def _():
        for peer in dap_peers(me_d, nd):
            greet({"dap": peer})

    @pl.when(jnp.logical_not(is_owner))
    def _():
        for r in ring_order(GROUP):
            greet({"dap": owner_of(lax.rem(my_m + r, GROUP), nd)})

    def push(src, dst, sem, peer):
        return pltpu.make_async_remote_copy(
            src_ref=src,
            dst_ref=dst,
            send_sem=send_sem.at[sem],
            recv_sem=recv_sem.at[sem],
            device_id=peer,
            device_id_type=pl.DeviceIdType.MESH,
        )

    def across_ch(src, dst, sem):
        for peer in ch_peers(me_s, ns):
            push(src.at[peer], dst.at[me_s], sem, {"ch": peer}).start()
        dst[me_s] = src[me_s]

    def await_ch(dst, sem):
        some = dst.at[pl.ds(0, ns - 1)]
        push(some, some, sem, {"ch": me_s}).wait_recv()

    def to_owners(src, dst, sem):
        def send(m):
            push(src.at[m], dst.at[me_d], sem, {"dap": owner_of(m, nd)}).start()

        for r in ring_order(GROUP)[:-1]:
            send(lax.rem(my_m + r, GROUP))

        @pl.when(is_owner)
        def _():
            dst[me_d] = src[my_m]

        @pl.when(jnp.logical_not(is_owner))
        def _():
            send(my_m)

    def await_owner(dst, sem):
        some = dst.at[pl.ds(0, nd - 1)]
        push(some, some, sem, {"dap": me_d}).wait_recv()

    def await_rows(dst, sem):
        @pl.when(is_owner)
        def _():
            some = dst.at[pl.ds(0, GROUP - 1)]
            push(some, some, sem, {"dap": me_d}).wait_recv()

        @pl.when(jnp.logical_not(is_owner))
        def _():
            push(dst, dst, sem, {"dap": me_d}).wait_recv()

    lane = lax.broadcasted_iota(jnp.int32, (1, CELLS), 1)
    place = lax.rem(lane, 16)
    used = jnp.logical_and(place < half, lane < rows * 32)
    first_half = lax.rem(lane, 32) < 16

    eye = (
        lax.broadcasted_iota(jnp.int32, (chans, chans), 0)
        == lax.broadcasted_iota(jnp.int32, (chans, chans), 1)
    ).astype(F32).astype(BF16)

    def cells_first(ref, slot):
        padded[slot] = jnp.zeros(padded.shape[1:], BF16)
        padded[slot, 0:rows, 0:columns, :] = ref[...]
        flat = padded[slot].reshape(CELLS, chans)
        turned = dot(eye, flat, ((1,), (1,)))
        spread = jnp.where(first_half, turned, pltpu.roll(turned, 1, 1))
        return jnp.where(used, spread, 0.0)

    def cells_last(turned):
        closed = jnp.where(
            lax.rem(lane, 32) < half, turned, pltpu.roll(turned, CELLS - 1, 1)
        )
        return closed.T.reshape(16, 32, chans)[0:rows, 0:columns, :].astype(BF16)

    loads[0].wait()
    xt = cells_first(x_ref, 0)
    center = jnp.mean(xt, axis=0, keepdims=True)
    spread = xt - center
    pair_scale = lax.rsqrt(jnp.mean(spread * spread, axis=0, keepdims=True) + EPSILON)
    nt = spread * pair_scale
    normed[...] = nt
    nh = nt.astype(BF16)

    residues = mask_ref.shape[1]
    total = nd * 16
    loads[2].wait()
    live[...] = jnp.zeros(live.shape, F32)
    live[:, 0:residues] = jnp.broadcast_to(mask_ref[...].astype(F32), (8, residues))
    flags = live[...].astype(BF16)

    def one_hot(hot):
        return jnp.where(hot, 1.0, 0.0).astype(BF16)

    at = lax.broadcasted_iota(jnp.int32, (total, 128), 0)
    lane_1 = lax.broadcasted_iota(jnp.int32, (total, 128), 1)
    row_flags = dot(
        flags, one_hot(jnp.logical_and(at == rows * me_d + lane_1, lane_1 < rows)), ((1,), (0,))
    )
    col_at = columns * me_s + half * (lax.rem(lane_1, 32) // 16) + lax.rem(lane_1, 16)
    col_flags = dot(
        flags, one_hot(jnp.logical_and(at == col_at, lax.rem(lane_1, 16) < half)), ((1,), (0,))
    )
    spot = lax.broadcasted_iota(jnp.int32, (128, CELLS), 0)
    row_of = lax.broadcasted_iota(jnp.int32, (128, CELLS), 1) // 32
    row_mask = dot(row_flags.astype(BF16), one_hot(spot == row_of), ((1,), (0,)))
    col_mask = jnp.concatenate([col_flags] * (CELLS // 128), axis=1)
    mask = (row_mask * col_mask)[0:1]

    def project(part):
        raw = dot(wp_ref[:, pl.ds(part * hidden, hidden)], nh, ((0,), (0,)))
        return raw

    def edge(part, slot):
        sig = jax.nn.sigmoid(project(part))
        val = project(part + 1)
        proj[part] = sig
        proj[part + 1] = val
        out1[slot] = (sig * val * mask).reshape(ns, GROUP, CELLS).astype(BF16)

    loads[1].wait()
    edge(0, 0)
    pl.semaphore_wait(barrier, ns - 1 + jnp.where(is_owner, nd - 1, GROUP))
    across_ch(out1.at[0], in1.at[0], 0)
    edge(2, 1)
    across_ch(out1.at[1], in1.at[1], 1)

    for load in loads[3:]:
        load.wait()
    gv = jax.nn.sigmoid(dot(wg_ref[...], nh, ((0,), (0,))))
    gate[...] = gv
    ct = cells_first(cot_ref, 1)
    cot[...] = ct
    gh = dot(wo_ref[...], (ct * gv).astype(BF16), ((1,), (0,)))
    ghid[...] = gh - jnp.mean(gh, axis=0, keepdims=True)

    for a in range(2):
        await_ch(in1.at[a], a)
        cells_to_rows(in1.at[a], mid, out2.at[a])
        to_owners(out2.at[a], own_in.at[a], 2 + a)

    width = ns * 32
    many = nd * 16

    def multiply(a, b, contract, buffer, back, sem):
        right = own_in[b].reshape(many, width)
        for h in range(2):
            if contract[0][0] == 1:
                part = own_in[a, pl.ds(h * nd // 2, nd // 2)].reshape(many // 2, width)
            else:
                part = own_in[a, :, :, pl.ds(h * width // 2, width // 2)].reshape(many, width // 2)
            value = dot(part, right, contract).astype(BF16)
            own_out[buffer, pl.ds(h * nd // 2, nd // 2)] = value.reshape(nd // 2, 16, width)
        for d in dap_peers(me_d, nd):
            push(own_out.at[buffer, d], in2.at[back, my_m], sem, {"dap": d}).start()
        in2[back, my_m] = own_out[buffer, me_d]

    @pl.when(is_owner)
    def _():
        await_owner(own_in.at[0], 2)
        await_owner(own_in.at[1], 3)
        multiply(0, 1, ((1,), (1,)), 0, 0, 4)

    await_rows(in2.at[0], 4)
    rows_to_cells(in2.at[0], mid, out1.at[2])
    across_ch(out1.at[2], in1.at[2], 5)
    await_ch(in1.at[2], 5)

    prod = in1[2].reshape(hidden, CELLS).astype(F32)
    away = prod - jnp.mean(prod, axis=0, keepdims=True)
    hidden_scale = lax.rsqrt(jnp.mean(away * away, axis=0, keepdims=True) + EPSILON)
    hn = away * hidden_scale
    gh_away = ghid[...]
    second = jnp.mean((gh_away) * hn, axis=0, keepdims=True)
    gprod = hidden_scale * (gh_away - hn * second)
    out1[3] = gprod.reshape(ns, GROUP, CELLS).astype(BF16)
    across_ch(out1.at[3], in1.at[3], 6)

    po = dot(wo_ref[...], hn.astype(BF16), ((0,), (0,)))
    gv = gate[...]
    glogit[...] = (cot[...] * po * gv * (1.0 - gv)).astype(BF16)
    upd_ref[...] = cells_last(gv * po)

    await_ch(in1.at[3], 6)
    cells_to_rows(in1.at[3], mid, out2.at[2])
    to_owners(out2.at[2], own_in.at[2], 7)

    @pl.when(is_owner)
    def _():
        await_owner(own_in.at[2], 7)
        multiply(2, 1, ((1,), (0,)), 1, 1, 8)
        multiply(2, 0, ((0,), (0,)), 2, 2, 9)

    base = dot(wg_ref[...], glogit[...], ((1,), (0,)))

    for a in range(2):
        await_rows(in2.at[1 + a], 8 + a)
        rows_to_cells(in2.at[1 + a], mid, out1.at[4 + a])
        across_ch(out1.at[4 + a], in1.at[4 + a], 10 + a)

    for a in range(2):
        await_ch(in1.at[4 + a], 10 + a)
        masked = in1[4 + a].reshape(hidden, CELLS).astype(F32) * mask
        sig = proj[2 * a]
        val = proj[2 * a + 1]
        to_sig = (masked * val * sig * (1.0 - sig)).astype(BF16)
        to_val = (masked * sig).astype(BF16)
        base = base + dot(wp_ref[:, pl.ds(2 * a * hidden, hidden)], to_sig, ((1,), (0,)))
        base = base + dot(wp_ref[:, pl.ds((2 * a + 1) * hidden, hidden)], to_val, ((1,), (0,)))

    nt = normed[...]
    first = jnp.mean(base, axis=0, keepdims=True)
    second = jnp.mean(base * nt, axis=0, keepdims=True)
    gpair_ref[...] = cells_last(pair_scale * (base - first - nt * second))

    def sent(ref, sem):
        push(ref, ref, sem, {"ch": me_s}).wait_send()

    few = pl.ds(0, ns - 1)
    for buffer, sem in ((0, 0), (1, 1), (2, 5), (3, 6), (4, 10), (5, 11)):
        sent(out1.at[buffer, few], sem)
    for buffer, sem in ((0, 2), (1, 3), (2, 7)):

        @pl.when(is_owner)
        def _():
            sent(out2.at[buffer, pl.ds(0, GROUP - 1)], sem)

        @pl.when(jnp.logical_not(is_owner))
        def _():
            sent(out2.at[buffer], sem)

    @pl.when(is_owner)
    def _():
        for buffer, sem in ((0, 4), (1, 8), (2, 9)):
            sent(own_out.at[buffer, pl.ds(0, nd - 1)], sem)


def to_hbm(upd, gpair, upd_hbm, gpair_hbm, sem):
    copies = [
        pltpu.make_async_copy(upd, upd_hbm, sem.at[0]),
        pltpu.make_async_copy(gpair, gpair_hbm, sem.at[1]),
    ]
    for copy in copies:
        copy.start()
    for copy in copies:
        copy.wait()


def on_device(nd, ns, pair_rep, residue_mask, w_proj, w_gate, w_out, cotangent):
    hidden, chans = w_out.shape
    vmem = pl.BlockSpec(memory_space=pltpu.VMEM)
    hbm = pl.BlockSpec(memory_space=pltpu.HBM)
    shape = jax.ShapeDtypeStruct(pair_rep.shape, BF16)
    width = ns * 32
    args = (pair_rep, cotangent, residue_mask[None, :], w_proj, w_gate, w_out)
    args = [pltpu.with_memory_space_constraint(a, pltpu.HBM) for a in args]
    results = pl.pallas_call(
        functools.partial(kernel, nd, ns),
        out_shape=(shape, shape),
        in_specs=[hbm] * 6,
        out_specs=(vmem, vmem),
        scratch_shapes=[pltpu.VMEM(a.shape, a.dtype) for a in args]
        + [
            pltpu.VMEM((2, 16, 32, chans), BF16),
            pltpu.VMEM((8, nd * 16), F32),
            pltpu.VMEM((4, hidden, CELLS), F32),
            pltpu.VMEM((chans, CELLS), F32),
            pltpu.VMEM((chans, CELLS), F32),
            pltpu.VMEM((chans, CELLS), F32),
            pltpu.VMEM((hidden, CELLS), F32),
            pltpu.VMEM((chans, CELLS), BF16),
            pltpu.VMEM((ns // 4, 16 * GROUP, 128), F32),
            pltpu.VMEM((6, ns, GROUP, CELLS), BF16),
            pltpu.VMEM((6, ns, GROUP, CELLS), BF16),
            pltpu.VMEM((3, GROUP, 16, width), BF16),
            pltpu.VMEM((3, GROUP, 16, width), BF16),
            pltpu.VMEM((3, nd, 16, width), BF16),
            pltpu.VMEM((3, nd, 16, width), BF16),
            pltpu.SemaphoreType.DMA((6,)),
            pltpu.SemaphoreType.DMA((12,)),
            pltpu.SemaphoreType.DMA((12,)),
        ],
        compiler_params=pltpu.CompilerParams(
            collective_id=0, has_side_effects=True, vmem_limit_bytes=50331648
        ),
    )(*args)
    return pl.pallas_call(
        to_hbm,
        out_shape=(shape, shape),
        in_specs=[vmem, vmem],
        out_specs=(hbm, hbm),
        scratch_shapes=[pltpu.SemaphoreType.DMA((2,))],
        compiler_params=pltpu.CompilerParams(vmem_limit_bytes=1024 * 1024),
    )(*results)


def solution(mesh):
    nd, ns = mesh.shape["dap"], mesh.shape["ch"]
    return jax.shard_map(
        functools.partial(on_device, nd, ns),
        mesh=mesh,
        in_specs=(P("dap", "ch", None), P(), P(), P(), P(), P("dap", "ch", None)),
        out_specs=(P("dap", "ch", None), P("dap", "ch", None)),
        check_vma=False,
    )
```

```python
import functools

import jax
import jax.numpy as jnp
from jax import lax
from jax.experimental import pallas as pl
from jax.experimental.pallas import tpu as pltpu
from jax.sharding import PartitionSpec as P

EPSILON = 1e-05
F32 = jnp.float32
BF16 = jnp.bfloat16
CELLS = 512
QUADS = CELLS // 128


def ring_order(size):
    return sorted(range(size), key=lambda r: -min(r, size - r))


def ch_peers(me, ch_size):
    ny = ch_size // 2
    steps = [(dy, dx) for dy in range(ny) for dx in range(2) if dy or dx]
    steps.sort(key=lambda p: -(min(p[0], ny - p[0]) + 2 * p[1]))
    y, x = me // 2, lax.rem(me, 2)
    return [2 * lax.rem(y + dy, ny) + lax.rem(x + dx, 2) for dy, dx in steps]


def dot(a, b, contract):
    return lax.dot_general(a, b, (contract, ((), ())), preferred_element_type=F32)


def swap_blocks(rows):
    block = lax.broadcasted_iota(jnp.int32, rows[0].shape, 1) // 32
    odd = lax.rem(block, 2) == 1
    high = block >= 2
    x0, x1, x2, x3 = rows
    z0 = jnp.where(odd, pltpu.roll(x1, 32, 1), x0)
    z1 = jnp.where(odd, x1, pltpu.roll(x0, 96, 1))
    z2 = jnp.where(odd, pltpu.roll(x3, 32, 1), x2)
    z3 = jnp.where(odd, x3, pltpu.roll(x2, 96, 1))
    return (
        jnp.where(high, pltpu.roll(z2, 64, 1), z0),
        jnp.where(high, pltpu.roll(z3, 64, 1), z1),
        jnp.where(high, z2, pltpu.roll(z0, 64, 1)),
        jnp.where(high, z3, pltpu.roll(z1, 64, 1)),
    )


def cells_to_rows(cells, first, count, mid, rows, place):
    group = cells.shape[1]
    for t in range(count // 4):
        for q in range(QUADS):
            lanes = pl.ds(q * 128, 128)
            moved = swap_blocks([cells[first + 4 * t + a, :, lanes].astype(F32) for a in range(4)])
            for b in range(4):
                mid[t, pl.ds(4 * q + b, group, stride=16), :] = moved[b]
    for t in range(count // 4):
        for m in range(group):
            rows[place(m), :, pl.ds(t * 128, 128)] = mid[t, pl.ds(16 * m, 16), :].astype(BF16)


def rows_to_cells(rows, place, mid, cells, first, count):
    group = cells.shape[1]
    for t in range(count // 4):
        for m in range(group):
            mid[t, pl.ds(16 * m, 16), :] = rows[place(m), :, pl.ds(t * 128, 128)].astype(F32)
    for t in range(count // 4):
        for q in range(QUADS):
            lanes = pl.ds(q * 128, 128)
            moved = swap_blocks([mid[t, pl.ds(4 * q + b, group, stride=16), :] for b in range(4)])
            for a in range(4):
                cells[first + 4 * t + a, :, lanes] = moved[a].astype(BF16)


def swap_leading(src, mid, dst):
    na, nb = src.shape[0], src.shape[1]
    for q in range(QUADS):
        lanes = pl.ds(q * 128, 128)
        for a in range(na):
            mid[q, pl.ds(a * nb, nb), :] = src[a, :, lanes].astype(F32)
        for b in range(nb):
            dst[b, :, lanes] = mid[q, pl.ds(b, na, stride=nb), :].astype(BF16)


def kernel(
    nd,
    ns,
    x_hbm,
    cot_hbm,
    mask_hbm,
    wp_hbm,
    wg_hbm,
    wo_hbm,
    upd_ref,
    gpair_ref,
    x_ref,
    cot_ref,
    mask_ref,
    wp_ref,
    wg_ref,
    wo_ref,
    padded,
    live,
    proj,
    normed,
    gate,
    cot,
    ghid,
    glogit,
    mid,
    ch_out,
    ch_in,
    row_out,
    row_in,
    own_in,
    own_out,
    z_out,
    z_in,
    col_out,
    col_in,
    own_cells_in,
    own_cells_out,
    load_sem,
    send_sem,
    recv_sem,
):
    rows, columns, chans = x_ref.shape
    half = columns // 2
    nz = nd // 4
    hidden = ns * nz
    me_d = lax.axis_index("dap")
    me_s = lax.axis_index("ch")
    my_x, my_z, my_core = me_d // (2 * nz), lax.rem(me_d // 2, nz), lax.rem(me_d, 2)
    is_owner = jnp.logical_and(my_core == 1, my_x == lax.rem(my_z + me_s // 2, 2))

    def at_dap(x, z, core):
        return 2 * nz * x + 2 * z + core

    def owner_of(z, s):
        return at_dap(lax.rem(z + s // 2, 2), z, 1)

    near_ch = ch_peers(me_s, ns)
    z_order = [lax.rem(my_z + r, nz) for r in ring_order(nz)]
    other_x = 1 - my_x
    dap_order = [
        at_dap(x, z, core)
        for z in z_order
        for x in (other_x, my_x)
        for core in (0, 1)
    ][:-1]
    quarters = [(other_x, 0), (other_x, 1), (my_x, 0), (my_x, 1)]

    loads = [
        pltpu.make_async_copy(src, dst, load_sem.at[n])
        for n, (src, dst) in enumerate(
            (
                (x_hbm, x_ref),
                (wp_hbm, wp_ref),
                (mask_hbm, mask_ref),
                (cot_hbm, cot_ref),
                (wg_hbm, wg_ref),
                (wo_hbm, wo_ref),
            )
        )
    ]
    for load in loads:
        load.start()

    barrier = pltpu.get_barrier_semaphore()

    def greet(peer):
        pl.semaphore_signal(
            barrier, inc=1, device_id=peer, device_id_type=pl.DeviceIdType.MESH
        )

    for s in near_ch:
        greet({"ch": s})
    for z in z_order[:-1]:
        greet({"dap": at_dap(my_x, z, my_core)})

    @pl.when(is_owner)
    def _():
        for d in dap_order:
            greet({"dap": d})
        for x, core in quarters:
            for s in near_ch:
                greet({"dap": at_dap(x, my_z, core), "ch": s})
        for x, core in quarters[:-1]:
            greet({"dap": at_dap(x, my_z, core), "ch": me_s})

    @pl.when(jnp.logical_not(is_owner))
    def _():
        for z in z_order:
            greet({"dap": owner_of(z, me_s)})
        for s in near_ch + [me_s]:
            greet({"dap": owner_of(my_z, s), "ch": s})

    greetings = (
        ns - 1 + nz - 1 + jnp.where(is_owner, nd - 1 + 4 * ns - 1, nz + ns)
    )

    def push(src, dst, sem, peer, arrival=None):
        return pltpu.make_async_remote_copy(
            src_ref=src,
            dst_ref=dst,
            send_sem=send_sem.at[sem],
            recv_sem=recv_sem.at[sem if arrival is None else arrival],
            device_id=peer,
            device_id_type=pl.DeviceIdType.MESH,
        )

    def await_slabs(ref, count, sem):
        some = ref.at[pl.ds(0, count)]
        push(some, some, sem, {"dap": me_d}).wait_recv()

    def await_all_but_mine(ref, sem):
        @pl.when(is_owner)
        def _():
            await_slabs(ref, ref.shape[0] - 1, sem)

        @pl.when(jnp.logical_not(is_owner))
        def _():
            await_slabs(ref, ref.shape[0], sem)

    def across_ch(n, sem):
        src, dst = ch_out.at[n], ch_in.at[n]
        for s in near_ch:
            push(src.at[s], dst.at[me_s], sem, {"ch": s}).start()
        dst[me_s] = src[me_s]

    def await_ch(n, sem):
        await_slabs(ch_in.at[n], ns - 1, sem)

    def across_z(n, sem):
        src, dst = z_out.at[n], z_in.at[n]
        for z in z_order[:-1]:
            push(src.at[z], dst.at[my_z], sem, {"dap": at_dap(my_x, z, my_core)}).start()
        dst[my_z] = src[my_z]

    def await_z(n, sem):
        await_slabs(z_in.at[n], nz - 1, sem)

    def rows_to_owners(n, a, sem):
        src, dst = row_out.at[n], own_in.at[a]

        def send(z):
            push(src.at[z], dst.at[me_d], sem, {"dap": owner_of(z, me_s)}).start()

        for z in z_order[:-1]:
            send(z)

        @pl.when(is_owner)
        def _():
            dst[me_d] = src[my_z]

        @pl.when(jnp.logical_not(is_owner))
        def _():
            send(my_z)

    def columns_to_owners(sem):
        quarter = 2 * my_x + my_core
        slot = quarter * ns + me_s

        def send(s):
            peer = {"dap": owner_of(my_z, s), "ch": s}
            push(col_out.at[s], own_cells_in.at[slot], sem, peer, 12 + quarter).start()

        for s in near_ch:
            send(s)

        @pl.when(is_owner)
        def _():
            own_cells_in[slot] = col_out[me_s]

        @pl.when(jnp.logical_not(is_owner))
        def _():
            send(me_s)

    lane = lax.broadcasted_iota(jnp.int32, (1, CELLS), 1)
    place = lax.rem(lane, 16)
    used = jnp.logical_and(place < half, lane < rows * 32)
    first_half = lax.rem(lane, 32) < 16

    eye = (
        lax.broadcasted_iota(jnp.int32, (chans, chans), 0)
        == lax.broadcasted_iota(jnp.int32, (chans, chans), 1)
    ).astype(F32).astype(BF16)

    def cells_first(ref, slot):
        padded[slot] = jnp.zeros(padded.shape[1:], BF16)
        padded[slot, 0:rows, 0:columns, :] = ref[...]
        flat = padded[slot].reshape(CELLS, chans)
        turned = dot(eye, flat, ((1,), (1,)))
        spread = jnp.where(first_half, turned, pltpu.roll(turned, 1, 1))
        return jnp.where(used, spread, 0.0)

    def cells_last(turned):
        closed = jnp.where(
            lax.rem(lane, 32) < half, turned, pltpu.roll(turned, CELLS - 1, 1)
        )
        return closed.T.reshape(16, 32, chans)[0:rows, 0:columns, :].astype(BF16)

    loads[0].wait()
    xt = cells_first(x_ref, 0)
    center = jnp.mean(xt, axis=0, keepdims=True)
    spread = xt - center
    pair_scale = lax.rsqrt(jnp.mean(spread * spread, axis=0, keepdims=True) + EPSILON)
    nt = spread * pair_scale
    normed[...] = nt
    nh = nt.astype(BF16)

    residues = mask_ref.shape[1]
    total = nd * 16
    loads[2].wait()
    live[...] = jnp.zeros(live.shape, F32)
    live[:, 0:residues] = jnp.broadcast_to(mask_ref[...].astype(F32), (8, residues))
    flags = live[...].astype(BF16)

    def one_hot(hot):
        return jnp.where(hot, 1.0, 0.0).astype(BF16)

    at = lax.broadcasted_iota(jnp.int32, (total, 128), 0)
    lane_1 = lax.broadcasted_iota(jnp.int32, (total, 128), 1)
    row_flags = dot(
        flags, one_hot(jnp.logical_and(at == rows * me_d + lane_1, lane_1 < rows)), ((1,), (0,))
    )
    col_at = columns * me_s + half * (lax.rem(lane_1, 32) // 16) + lax.rem(lane_1, 16)
    col_flags = dot(
        flags, one_hot(jnp.logical_and(at == col_at, lax.rem(lane_1, 16) < half)), ((1,), (0,))
    )
    spot = lax.broadcasted_iota(jnp.int32, (128, CELLS), 0)
    row_of = lax.broadcasted_iota(jnp.int32, (128, CELLS), 1) // 32
    row_mask = dot(row_flags.astype(BF16), one_hot(spot == row_of), ((1,), (0,)))
    col_mask = jnp.concatenate([col_flags] * (CELLS // 128), axis=1)
    mask = (row_mask * col_mask)[0:1]

    def project(part):
        raw = dot(wp_ref[:, pl.ds(part * hidden, hidden)], nh, ((0,), (0,)))
        return raw

    def edge(part):
        sig = jax.nn.sigmoid(project(part))
        val = project(part + 1)
        proj[part] = sig
        proj[part + 1] = val
        return sig * val * mask

    loads[1].wait()
    ch_out[0] = edge(0).reshape(ns, nz, CELLS).astype(BF16)
    right = edge(2)
    for q in range(QUADS):
        lanes = slice(q * 128, q * 128 + 128)
        mid[q, 0:hidden, :] = right[:, lanes]
        for z in range(nz):
            z_out[0, z, :, lanes] = mid[q, pl.ds(z, ns, stride=nz), :].astype(BF16)
    pl.semaphore_wait(barrier, greetings)
    across_z(0, 1)
    across_ch(0, 0)

    for load in loads[3:]:
        load.wait()
    gv = jax.nn.sigmoid(dot(wg_ref[...], nh, ((0,), (0,))))
    gate[...] = gv
    ct = cells_first(cot_ref, 1)
    cot[...] = ct
    gh = dot(wo_ref[...], (ct * gv).astype(BF16), ((1,), (0,)))
    ghid[...] = gh - jnp.mean(gh, axis=0, keepdims=True)

    await_z(0, 1)
    swap_leading(z_in.at[0], mid, col_out)
    columns_to_owners(3)
    await_ch(0, 0)
    cells_to_rows(ch_in.at[0], 0, ns, mid, row_out.at[0], lambda m: m)
    rows_to_owners(0, 0, 2)

    width = ns * 32
    many = nd * 16

    def multiply(a, b, contract, n):
        right = own_in[b].reshape(many, width)
        for h in range(2):
            if contract[0][0] == 1:
                part = own_in[a, pl.ds(h * nd // 2, nd // 2)].reshape(many // 2, width)
            else:
                part = own_in[a, :, :, pl.ds(h * width // 2, width // 2)].reshape(many, width // 2)
            value = dot(part, right, contract).astype(BF16)
            own_out[n, pl.ds(h * nd // 2, nd // 2)] = value.reshape(nd // 2, 16, width)

    def rows_back(n, sem):
        src, dst = own_out.at[n], row_in.at[n]
        for d in dap_order:
            push(src.at[d], dst.at[my_z], sem, {"dap": d}).start()
        dst[my_z] = src[me_d]

    def columns_back(n, sem):
        for g, (x, core) in enumerate(quarters):
            rows_to_cells(
                own_out.at[n],
                lambda z, x=x, core=core: at_dap(x, z, core),
                mid,
                own_cells_out,
                g * ns,
                ns,
            )
            d = at_dap(x, my_z, core)
            for s in near_ch + ([me_s] if g < 3 else []):
                push(
                    own_cells_out.at[g * ns + s], col_in.at[me_s], sem, {"dap": d, "ch": s}
                ).start()
        col_in[me_s] = own_cells_out[3 * ns + me_s]

    @pl.when(is_owner)
    def _():
        def arrived(x, core, count):
            quarter = 2 * x + core
            await_slabs(own_cells_in, count, 12 + quarter)
            cells_to_rows(
                own_cells_in,
                quarter * ns,
                ns,
                mid,
                own_in.at[1],
                lambda z: at_dap(x, z, core),
            )

        arrived(my_x, 1, ns - 1)

        @pl.loop(0, 3)
        def _(r):
            arrived(jnp.where(r == 0, my_x, other_x), lax.rem(r, 2), ns)

        await_slabs(own_in.at[0], nd - 1, 2)
        multiply(0, 1, ((1,), (1,)), 0)
        rows_back(0, 4)

    await_all_but_mine(row_in.at[0], 4)
    rows_to_cells(row_in.at[0], lambda m: m, mid, ch_out.at[1], 0, ns)
    across_ch(1, 5)
    await_ch(1, 5)

    prod = ch_in[1].reshape(hidden, CELLS).astype(F32)
    away = prod - jnp.mean(prod, axis=0, keepdims=True)
    hidden_scale = lax.rsqrt(jnp.mean(away * away, axis=0, keepdims=True) + EPSILON)
    hn = away * hidden_scale
    gh_away = ghid[...]
    second = jnp.mean((gh_away) * hn, axis=0, keepdims=True)
    gprod = hidden_scale * (gh_away - hn * second)
    ch_out[2] = gprod.reshape(ns, nz, CELLS).astype(BF16)
    across_ch(2, 6)

    po = dot(wo_ref[...], hn.astype(BF16), ((0,), (0,)))
    gv = gate[...]
    glogit[...] = (cot[...] * po * gv * (1.0 - gv)).astype(BF16)
    upd_ref[...] = cells_last(gv * po)

    await_ch(2, 6)
    cells_to_rows(ch_in.at[2], 0, ns, mid, row_out.at[1], lambda m: m)
    rows_to_owners(1, 2, 7)

    @pl.when(is_owner)
    def _():
        await_slabs(own_in.at[2], nd - 1, 7)
        multiply(2, 1, ((1,), (0,)), 1)
        rows_back(1, 8)
        multiply(2, 0, ((0,), (0,)), 2)
        columns_back(2, 9)

    base = dot(wg_ref[...], glogit[...], ((1,), (0,)))

    def through(base, part, back):
        masked = back * mask
        sig = proj[part]
        val = proj[part + 1]
        to_sig = (masked * val * sig * (1.0 - sig)).astype(BF16)
        to_val = (masked * sig).astype(BF16)
        base = base + dot(wp_ref[:, pl.ds(part * hidden, hidden)], to_sig, ((1,), (0,)))
        return base + dot(wp_ref[:, pl.ds((part + 1) * hidden, hidden)], to_val, ((1,), (0,)))

    await_all_but_mine(row_in.at[1], 8)
    rows_to_cells(row_in.at[1], lambda m: m, mid, ch_out.at[3], 0, ns)
    across_ch(3, 10)
    await_all_but_mine(col_in, 9)
    swap_leading(col_in, mid, z_out.at[1])
    across_z(1, 11)
    await_ch(3, 10)
    base = through(base, 0, ch_in[3].reshape(hidden, CELLS).astype(F32))
    await_z(1, 11)
    for q in range(QUADS):
        lanes = slice(q * 128, q * 128 + 128)
        for z in range(nz):
            mid[q, pl.ds(z, ns, stride=nz), :] = z_in[1, z, :, lanes].astype(F32)
    back = jnp.concatenate([mid[q, 0:hidden, :] for q in range(QUADS)], axis=1)
    base = through(base, 2, back)

    nt = normed[...]
    first = jnp.mean(base, axis=0, keepdims=True)
    second = jnp.mean(base * nt, axis=0, keepdims=True)
    gpair_ref[...] = cells_last(pair_scale * (base - first - nt * second))

    def sent(ref, count, sem):
        some = ref.at[pl.ds(0, count)]
        push(some, some, sem, {"dap": me_d}).wait_send()

    for n, sem in ((0, 0), (1, 5), (2, 6), (3, 10)):
        sent(ch_out.at[n], ns - 1, sem)
    for n, sem in ((0, 1), (1, 11)):
        sent(z_out.at[n], nz - 1, sem)

    @pl.when(is_owner)
    def _():
        sent(row_out.at[0], nz - 1, 2)
        sent(row_out.at[1], nz - 1, 7)
        sent(col_out, ns - 1, 3)
        sent(own_out.at[0], nd - 1, 4)
        sent(own_out.at[1], nd - 1, 8)
        sent(own_cells_out, 4 * ns - 1, 9)

    @pl.when(jnp.logical_not(is_owner))
    def _():
        sent(row_out.at[0], nz, 2)
        sent(row_out.at[1], nz, 7)
        sent(col_out, ns, 3)


def to_hbm(upd, gpair, upd_hbm, gpair_hbm, sem):
    copies = [
        pltpu.make_async_copy(upd, upd_hbm, sem.at[0]),
        pltpu.make_async_copy(gpair, gpair_hbm, sem.at[1]),
    ]
    for copy in copies:
        copy.start()
    for copy in copies:
        copy.wait()


def on_device(nd, ns, pair_rep, residue_mask, w_proj, w_gate, w_out, cotangent):
    hidden, chans = w_out.shape
    vmem = pl.BlockSpec(memory_space=pltpu.VMEM)
    hbm = pl.BlockSpec(memory_space=pltpu.HBM)
    shape = jax.ShapeDtypeStruct(pair_rep.shape, BF16)
    width = ns * 32
    nz = nd // 4
    args = (pair_rep, cotangent, residue_mask[None, :], w_proj, w_gate, w_out)
    args = [pltpu.with_memory_space_constraint(a, pltpu.HBM) for a in args]
    results = pl.pallas_call(
        functools.partial(kernel, nd, ns),
        out_shape=(shape, shape),
        in_specs=[hbm] * 6,
        out_specs=(vmem, vmem),
        scratch_shapes=[pltpu.VMEM(a.shape, a.dtype) for a in args]
        + [
            pltpu.VMEM((2, 16, 32, chans), BF16),
            pltpu.VMEM((8, nd * 16), F32),
            pltpu.VMEM((4, hidden, CELLS), F32),
            pltpu.VMEM((chans, CELLS), F32),
            pltpu.VMEM((chans, CELLS), F32),
            pltpu.VMEM((chans, CELLS), F32),
            pltpu.VMEM((hidden, CELLS), F32),
            pltpu.VMEM((chans, CELLS), BF16),
            pltpu.VMEM((QUADS, 16 * nz, 128), F32),
            pltpu.VMEM((4, ns, nz, CELLS), BF16),
            pltpu.VMEM((4, ns, nz, CELLS), BF16),
            pltpu.VMEM((2, nz, 16, width), BF16),
            pltpu.VMEM((2, nz, 16, width), BF16),
            pltpu.VMEM((3, nd, 16, width), BF16),
            pltpu.VMEM((3, nd, 16, width), BF16),
            pltpu.VMEM((2, nz, ns, CELLS), BF16),
            pltpu.VMEM((2, nz, ns, CELLS), BF16),
            pltpu.VMEM((ns, nz, CELLS), BF16),
            pltpu.VMEM((ns, nz, CELLS), BF16),
            pltpu.VMEM((4 * ns, nz, CELLS), BF16),
            pltpu.VMEM((4 * ns, nz, CELLS), BF16),
            pltpu.SemaphoreType.DMA((6,)),
            pltpu.SemaphoreType.DMA((12,)),
            pltpu.SemaphoreType.DMA((16,)),
        ],
        compiler_params=pltpu.CompilerParams(
            collective_id=0, has_side_effects=True, vmem_limit_bytes=50331648
        ),
    )(*args)
    return pl.pallas_call(
        to_hbm,
        out_shape=(shape, shape),
        in_specs=[vmem, vmem],
        out_specs=(hbm, hbm),
        scratch_shapes=[pltpu.SemaphoreType.DMA((2,))],
        compiler_params=pltpu.CompilerParams(vmem_limit_bytes=1024 * 1024),
    )(*results)


def solution(mesh):
    nd, ns = mesh.shape["dap"], mesh.shape["ch"]
    return jax.shard_map(
        functools.partial(on_device, nd, ns),
        mesh=mesh,
        in_specs=(P("dap", "ch", None), P(), P(), P(), P(), P("dap", "ch", None)),
        out_specs=(P("dap", "ch", None), P("dap", "ch", None)),
        check_vma=False,
    )
```

```python
import functools

import jax
import jax.numpy as jnp
from jax import lax
from jax.experimental import pallas as pl
from jax.experimental.pallas import tpu as pltpu
from jax.sharding import PartitionSpec as P

EPSILON = 1e-05
F32 = jnp.float32
BF16 = jnp.bfloat16
CELLS = 512
QUADS = CELLS // 128
LEFT, RIGHT, PRODUCT, GRAD, GRAD_LEFT, GRAD_RIGHT = range(6)
BY_Z = (RIGHT, GRAD_RIGHT)


def ring_order(size):
    return sorted(range(size), key=lambda r: -min(r, size - r))


def ch_peers(me, ch_size):
    ny = ch_size // 2
    steps = [(dy, dx) for dy in range(ny) for dx in range(2) if dy or dx]
    steps.sort(key=lambda p: -(min(p[0], ny - p[0]) + 2 * p[1]))
    y, x = me // 2, lax.rem(me, 2)
    return [2 * lax.rem(y + dy, ny) + lax.rem(x + dx, 2) for dy, dx in steps]


def dot(a, b, contract):
    return lax.dot_general(a, b, (contract, ((), ())), preferred_element_type=F32)


def swap_blocks(rows):
    block = lax.broadcasted_iota(jnp.int32, rows[0].shape, 1) // 32
    odd = lax.rem(block, 2) == 1
    high = block >= 2
    x0, x1, x2, x3 = rows
    z0 = jnp.where(odd, pltpu.roll(x1, 32, 1), x0)
    z1 = jnp.where(odd, x1, pltpu.roll(x0, 96, 1))
    z2 = jnp.where(odd, pltpu.roll(x3, 32, 1), x2)
    z3 = jnp.where(odd, x3, pltpu.roll(x2, 96, 1))
    return (
        jnp.where(high, pltpu.roll(z2, 64, 1), z0),
        jnp.where(high, pltpu.roll(z3, 64, 1), z1),
        jnp.where(high, z2, pltpu.roll(z0, 64, 1)),
        jnp.where(high, z3, pltpu.roll(z1, 64, 1)),
    )


def cells_to_rows(cells, first, count, mid, rows, place):
    group = cells.shape[1]
    for t in range(count // 4):
        for q in range(QUADS):
            lanes = pl.ds(q * 128, 128)
            moved = swap_blocks([cells[first + 4 * t + a, :, lanes].astype(F32) for a in range(4)])
            for b in range(4):
                mid[t, pl.ds(4 * q + b, group, stride=16), :] = moved[b]
    for t in range(count // 4):
        for m in range(group):
            rows[place(m), :, pl.ds(t * 128, 128)] = mid[t, pl.ds(16 * m, 16), :].astype(BF16)


def rows_to_cells(rows, place, mid, cells, first, count):
    group = cells.shape[1]
    for t in range(count // 4):
        for m in range(group):
            mid[t, pl.ds(16 * m, 16), :] = rows[place(m), :, pl.ds(t * 128, 128)].astype(F32)
    for t in range(count // 4):
        for q in range(QUADS):
            lanes = pl.ds(q * 128, 128)
            moved = swap_blocks([mid[t, pl.ds(4 * q + b, group, stride=16), :] for b in range(4)])
            for a in range(4):
                cells[first + 4 * t + a, :, lanes] = moved[a].astype(BF16)


def swap_leading(src, mid, dst):
    na, nb = src.shape[0], src.shape[1]
    for q in range(QUADS):
        lanes = pl.ds(q * 128, 128)
        for a in range(na):
            mid[q, pl.ds(a * nb, nb), :] = src[a, :, lanes].astype(F32)
        for b in range(nb):
            dst[b, :, lanes] = mid[q, pl.ds(b, na, stride=nb), :].astype(BF16)


def kernel(
    nd,
    ns,
    x_hbm,
    cot_hbm,
    mask_hbm,
    wp_hbm,
    wg_hbm,
    wo_hbm,
    upd_ref,
    gpair_ref,
    x_ref,
    cot_ref,
    mask_ref,
    wp_ref,
    wg_ref,
    wo_ref,
    padded,
    live,
    proj,
    normed,
    gate,
    cot,
    ghid,
    glogit,
    mid,
    ch_out,
    ch_in,
    row_out,
    row_in,
    own_in,
    own_out,
    z_out,
    z_in,
    col_out,
    col_in,
    own_cells,
    cell_tiles,
    own_tiles,
    own_mid,
    flat,
    load_sem,
    send_sem,
    recv_sem,
):
    rows, columns, chans = x_ref.shape
    half = columns // 2
    nz = nd // 4
    hidden = ns * nz
    me_d = lax.axis_index("dap")
    me_s = lax.axis_index("ch")
    my_x, my_z, my_core = me_d // (2 * nz), lax.rem(me_d // 2, nz), lax.rem(me_d, 2)
    is_owner = jnp.logical_and(my_core == 1, my_x == lax.rem(my_z + me_s // 2, 2))

    def at_dap(x, z, core):
        return 2 * nz * x + 2 * z + core

    def owner_of(z, s):
        return at_dap(lax.rem(z + s // 2, 2), z, 1)

    near_ch = ch_peers(me_s, ns)
    z_order = [lax.rem(my_z + r, nz) for r in ring_order(nz)]
    other_x = 1 - my_x
    dap_order = [
        at_dap(x, z, core)
        for z in z_order
        for x in (other_x, my_x)
        for core in (0, 1)
    ][:-1]
    quarters = [(other_x, 0), (other_x, 1), (my_x, 0), (my_x, 1)]

    loads = [
        pltpu.make_async_copy(src, dst, load_sem.at[n])
        for n, (src, dst) in enumerate(
            (
                (x_hbm, x_ref),
                (wp_hbm, wp_ref),
                (mask_hbm, mask_ref),
                (cot_hbm, cot_ref),
                (wg_hbm, wg_ref),
                (wo_hbm, wo_ref),
            )
        )
    ]
    for load in loads:
        load.start()

    barrier = pltpu.get_barrier_semaphore()

    def greet(peer):
        pl.semaphore_signal(
            barrier, inc=1, device_id=peer, device_id_type=pl.DeviceIdType.MESH
        )

    for s in near_ch:
        greet({"ch": s})
    for z in z_order[:-1]:
        greet({"dap": at_dap(my_x, z, my_core)})

    @pl.when(is_owner)
    def _():
        for d in dap_order:
            greet({"dap": d})
        for x, core in quarters:
            for s in near_ch:
                greet({"dap": at_dap(x, my_z, core), "ch": s})
        for x, core in quarters[:-1]:
            greet({"dap": at_dap(x, my_z, core), "ch": me_s})

    @pl.when(jnp.logical_not(is_owner))
    def _():
        for z in z_order:
            greet({"dap": owner_of(z, me_s)})
        for s in near_ch + [me_s]:
            greet({"dap": owner_of(my_z, s), "ch": s})

    greetings = (
        ns - 1 + nz - 1 + jnp.where(is_owner, nd - 1 + 4 * ns - 1, nz + ns)
    )

    def push(src, dst, sem, peer, arrival=None):
        return pltpu.make_async_remote_copy(
            src_ref=src,
            dst_ref=dst,
            send_sem=send_sem.at[sem],
            recv_sem=recv_sem.at[sem if arrival is None else arrival],
            device_id=peer,
            device_id_type=pl.DeviceIdType.MESH,
        )

    def await_slabs(ref, count, sem):
        some = ref.at[pl.ds(0, count)]
        push(some, some, sem, {"dap": me_d}).wait_recv()

    def await_all_but_mine(ref, sem):
        @pl.when(is_owner)
        def _():
            await_slabs(ref, ref.shape[0] - 1, sem)

        @pl.when(jnp.logical_not(is_owner))
        def _():
            await_slabs(ref, ref.shape[0], sem)

    def across_ch(n):
        src, dst, sem = ch_out.at[n], ch_in.at[n], 8 * n
        for s in near_ch:
            push(src.at[s], dst.at[me_s], sem, {"ch": s}).start()
        dst[me_s] = src[me_s]

    def across_z(n):
        src, dst, sem = z_out.at[n], z_in.at[n], 8 * n
        for z in z_order[:-1]:
            push(src.at[z], dst.at[my_z], sem, {"dap": at_dap(my_x, z, my_core)}).start()
        dst[my_z] = src[my_z]

    def rows_to_owners(n, a):
        src, dst, sem = row_out.at[n], own_in.at[a], 8 * n + 1

        def send(z):
            push(src.at[z], dst.at[me_d], sem, {"dap": owner_of(z, me_s)}).start()

        for z in z_order[:-1]:
            send(z)

        @pl.when(is_owner)
        def _():
            dst[me_d] = src[my_z]

        @pl.when(jnp.logical_not(is_owner))
        def _():
            send(my_z)

    def columns_to_owners(n):
        quarter = 2 * my_x + my_core
        slot = quarter * ns + me_s
        sem = 8 * n + 1

        def send(s):
            peer = {"dap": owner_of(my_z, s), "ch": s}
            push(col_out.at[n, s], own_cells.at[n, slot], sem, peer, sem + quarter).start()

        for s in near_ch:
            send(s)

        @pl.when(is_owner)
        def _():
            own_cells[n, slot] = col_out[n, me_s]

        @pl.when(jnp.logical_not(is_owner))
        def _():
            send(me_s)

    def leave(n, value):
        if n in BY_Z:
            for q in range(QUADS):
                lanes = slice(q * 128, q * 128 + 128)
                mid[q, 0:hidden, :] = value[:, lanes]
                for z in range(nz):
                    z_out[n, z, :, lanes] = mid[q, pl.ds(z, ns, stride=nz), :].astype(BF16)
        else:
            ch_out[n] = value.reshape(ns, nz, CELLS).astype(BF16)

    def across(n):
        if n in BY_Z:
            across_z(n)
        else:
            across_ch(n)

    def forward(n, a):
        if n in BY_Z:
            await_slabs(z_in.at[n], nz - 1, 8 * n)
            swap_leading(z_in.at[n], mid, col_out.at[n])
            columns_to_owners(n)
        else:
            await_slabs(ch_in.at[n], ns - 1, 8 * n)
            cells_to_rows(ch_in.at[n], 0, ns, mid, row_out.at[n], lambda m: m)
            rows_to_owners(n, a)

    def gathered(n, a):
        if n not in BY_Z:
            await_slabs(own_in.at[a], nd - 1, 8 * n + 1)
            return

        def arrived(x, core, count):
            quarter = 2 * x + core
            await_slabs(own_cells.at[n], count, 8 * n + 1 + quarter)
            cells_to_rows(
                own_cells.at[n],
                quarter * ns,
                ns,
                mid,
                own_in.at[a],
                lambda z: at_dap(x, z, core),
            )

        arrived(my_x, 1, ns - 1)

        @pl.loop(0, 3)
        def _(r):
            arrived(jnp.where(r == 0, my_x, other_x), lax.rem(r, 2), ns)

    def multiply(a, b, contract, c):
        right = own_in[b].reshape(many, width)
        for h in range(2):
            if contract[0][0] == 1:
                part = own_in[a, pl.ds(h * nd // 2, nd // 2)].reshape(many // 2, width)
            else:
                part = own_in[a, :, :, pl.ds(h * width // 2, width // 2)].reshape(many, width // 2)
            value = dot(part, right, contract)
            if c is None:
                for t in range(ns // 4):
                    own_mid[t, pl.ds(h * many // 2, many // 2), :] = value[:, t * 128 : t * 128 + 128]
            else:
                value = value.astype(BF16).reshape(nd // 2, 16, width)
                own_out[c, pl.ds(h * nd // 2, nd // 2)] = value

    tiles = ns // 4
    my_tile = me_s // 4
    me = me_d * ns + me_s

    def tile_at(step):
        shift = jnp.where(lax.rem(step, 2) == 1, -((step + 1) // 2), step // 2)
        return lax.rem(my_tile + tiles // 2 + shift, tiles)

    def scatter_product():
        mine = me_s * nz + my_z

        @pl.loop(0, tiles)
        def _(step):
            t = tile_at(step)
            for p in range(nd // 2):
                moved = swap_blocks([own_mid[t, pl.ds(32 * p + b, 8, stride=4), :] for b in range(4)])
                for a in range(4):
                    line = moved[a].astype(BF16)
                    for core in range(2):
                        own_tiles[0, (2 * p + core) * ns + 4 * t + a] = line[
                            4 * core : 4 * core + 4
                        ]
            for d in dap_order + [me_d]:
                for a in range(4):
                    s = 4 * t + a

                    def send(d=d, s=s):
                        push(
                            own_tiles.at[0, d * ns + s],
                            cell_tiles.at[0, mine],
                            8 * PRODUCT,
                            {"dap": d, "ch": s},
                        ).start()

                    if d is me_d:
                        pl.when(s != me_s)(send)
                    else:
                        send()

        cell_tiles[0, mine] = own_tiles[0, me]

    def product_at_cells():
        await_all_but_mine(cell_tiles.at[0], 8 * PRODUCT)

        for c in range(hidden):
            flat[pl.ds(4 * c, 4), :] = cell_tiles[0, c].astype(F32)

        return jnp.concatenate(
            [flat[pl.ds(q, hidden, stride=QUADS), :] for q in range(QUADS)], axis=1
        )

    def send_gradient(value):
        for q in range(QUADS):
            flat[pl.ds(q, hidden, stride=QUADS), :] = value[:, q * 128 : q * 128 + 128]

        for c in range(hidden // 2):
            pair = flat[pl.ds(8 * c, 8), :].astype(BF16)
            cell_tiles[1, 2 * c] = pair[0:4]
            cell_tiles[1, 2 * c + 1] = pair[4:8]

        ny = ns // 2
        steps = [(dz, dy, dx) for dz in range(nz) for dy in range(ny) for dx in range(2)]
        steps.sort(key=lambda p: -(min(p[0], nz - p[0]) + min(p[1], ny - p[1]) + 2 * p[2]))
        for dz, dy, dx in steps:
            z = lax.rem(my_z + dz, nz)
            s = 2 * lax.rem(me_s // 2 + dy, ny) + lax.rem(me_s + dx, 2)

            def send(z=z, s=s):
                push(
                    cell_tiles.at[1, s * nz + z],
                    own_tiles.at[1, me],
                    8 * GRAD,
                    {"dap": owner_of(z, s), "ch": s},
                    8 * GRAD + 1 + my_tile,
                ).start()

            if dz or dy or dx:
                send()
            else:
                pl.when(jnp.logical_not(is_owner))(send)

        @pl.when(is_owner)
        def _():
            own_tiles[1, me] = cell_tiles[1, me_s * nz + my_z]

    def gather_gradient(a):
        @pl.loop(0, tiles)
        def _(step):
            t = tile_at(tiles - 1 - step)

            def arrived(count):
                some = own_tiles.at[1, pl.ds(0, count)]
                push(some, some, 8 * GRAD, {"dap": me_d}, 8 * GRAD + 1 + t).wait_recv()

            pl.when(t == my_tile)(lambda: arrived(4 * nd - 1))
            pl.when(t != my_tile)(lambda: arrived(4 * nd))
            for p in range(nd // 2):
                got = [
                    jnp.concatenate(
                        [
                            own_tiles[1, (2 * p + core) * ns + 4 * t + e].astype(F32)
                            for core in range(2)
                        ],
                        axis=0,
                    )
                    for e in range(4)
                ]
                for b, rows in enumerate(swap_blocks(got)):
                    own_mid[t, pl.ds(32 * p + b, 8, stride=4), :] = rows
            lanes = pl.ds(pl.multiple_of(t * 128, 128), 128)
            for d in range(nd):
                own_in[a, d, :, lanes] = own_mid[t, pl.ds(16 * d, 16), :].astype(BF16)

    def give_back(n, c):
        if n not in BY_Z:
            src, dst = own_out.at[c], row_in.at[n]
            for d in dap_order:
                push(src.at[d], dst.at[my_z], 8 * n + 1, {"dap": d}).start()
            dst[my_z] = src[me_d]
            return
        for g, (x, core) in enumerate(quarters):
            rows_to_cells(
                own_out.at[c],
                lambda z, x=x, core=core: at_dap(x, z, core),
                mid,
                own_cells.at[n],
                g * ns,
                ns,
            )
            d = at_dap(x, my_z, core)
            for s in near_ch + ([me_s] if g < 3 else []):
                push(
                    own_cells.at[n, g * ns + s],
                    col_in.at[n, me_s],
                    8 * n + 1,
                    {"dap": d, "ch": s},
                ).start()
        col_in[n, me_s] = own_cells[n, 3 * ns + me_s]

    def pass_on(n):
        if n in BY_Z:
            await_all_but_mine(col_in.at[n], 8 * n + 1)
            swap_leading(col_in.at[n], mid, z_out.at[n])
        else:
            await_all_but_mine(row_in.at[n], 8 * n + 1)
            rows_to_cells(row_in.at[n], lambda m: m, mid, ch_out.at[n], 0, ns)
        across(n)

    def arrive(n):
        if n not in BY_Z:
            await_slabs(ch_in.at[n], ns - 1, 8 * n)
            return ch_in[n].reshape(hidden, CELLS).astype(F32)
        await_slabs(z_in.at[n], nz - 1, 8 * n)
        for q in range(QUADS):
            for z in range(nz):
                mid[q, pl.ds(z, ns, stride=nz), :] = z_in[n, z, :, pl.ds(q * 128, 128)].astype(F32)
        return jnp.concatenate([mid[q, 0:hidden, :] for q in range(QUADS)], axis=1)

    width = ns * 32
    many = nd * 16

    lane = lax.broadcasted_iota(jnp.int32, (1, CELLS), 1)
    place = lax.rem(lane, 16)
    used = jnp.logical_and(place < half, lane < rows * 32)
    first_half = lax.rem(lane, 32) < 16

    eye = (
        lax.broadcasted_iota(jnp.int32, (chans, chans), 0)
        == lax.broadcasted_iota(jnp.int32, (chans, chans), 1)
    ).astype(F32).astype(BF16)

    def cells_first(ref, slot):
        padded[slot] = jnp.zeros(padded.shape[1:], BF16)
        padded[slot, 0:rows, 0:columns, :] = ref[...]
        flat = padded[slot].reshape(CELLS, chans)
        turned = dot(eye, flat, ((1,), (1,)))
        spread = jnp.where(first_half, turned, pltpu.roll(turned, 1, 1))
        return jnp.where(used, spread, 0.0)

    def cells_last(turned):
        closed = jnp.where(
            lax.rem(lane, 32) < half, turned, pltpu.roll(turned, CELLS - 1, 1)
        )
        return closed.T.reshape(16, 32, chans)[0:rows, 0:columns, :].astype(BF16)

    loads[0].wait()
    xt = cells_first(x_ref, 0)
    center = jnp.mean(xt, axis=0, keepdims=True)
    spread = xt - center
    pair_scale = lax.rsqrt(jnp.mean(spread * spread, axis=0, keepdims=True) + EPSILON)
    nt = spread * pair_scale
    normed[...] = nt
    nh = nt.astype(BF16)

    residues = mask_ref.shape[1]
    total = nd * 16
    loads[2].wait()
    live[...] = jnp.zeros(live.shape, F32)
    live[:, 0:residues] = jnp.broadcast_to(mask_ref[...].astype(F32), (8, residues))
    flags = live[...].astype(BF16)

    def one_hot(hot):
        return jnp.where(hot, 1.0, 0.0).astype(BF16)

    at = lax.broadcasted_iota(jnp.int32, (total, 128), 0)
    lane_1 = lax.broadcasted_iota(jnp.int32, (total, 128), 1)
    row_flags = dot(
        flags, one_hot(jnp.logical_and(at == rows * me_d + lane_1, lane_1 < rows)), ((1,), (0,))
    )
    col_at = columns * me_s + half * (lax.rem(lane_1, 32) // 16) + lax.rem(lane_1, 16)
    col_flags = dot(
        flags, one_hot(jnp.logical_and(at == col_at, lax.rem(lane_1, 16) < half)), ((1,), (0,))
    )
    spot = lax.broadcasted_iota(jnp.int32, (128, CELLS), 0)
    row_of = lax.broadcasted_iota(jnp.int32, (128, CELLS), 1) // 32
    row_mask = dot(row_flags.astype(BF16), one_hot(spot == row_of), ((1,), (0,)))
    col_mask = jnp.concatenate([col_flags] * (CELLS // 128), axis=1)
    mask = (row_mask * col_mask)[0:1]

    def project(part):
        raw = dot(wp_ref[:, pl.ds(part * hidden, hidden)], nh, ((0,), (0,)))
        return raw

    def edge(part):
        sig = jax.nn.sigmoid(project(part))
        val = project(part + 1)
        proj[part] = sig
        proj[part + 1] = val
        return sig * val * mask

    loads[1].wait()
    leave(LEFT, edge(0))
    leave(RIGHT, edge(2))
    pl.semaphore_wait(barrier, greetings)
    across(RIGHT)
    across(LEFT)

    for load in loads[3:]:
        load.wait()
    gv = jax.nn.sigmoid(dot(wg_ref[...], nh, ((0,), (0,))))
    gate[...] = gv
    ct = cells_first(cot_ref, 1)
    cot[...] = ct
    gh = dot(wo_ref[...], (ct * gv).astype(BF16), ((1,), (0,)))
    ghid[...] = gh - jnp.mean(gh, axis=0, keepdims=True)

    forward(RIGHT, 1)
    forward(LEFT, 0)

    @pl.when(is_owner)
    def _():
        gathered(RIGHT, 1)
        gathered(LEFT, 0)
        multiply(0, 1, ((1,), (1,)), None)
        scatter_product()

    prod = product_at_cells()
    away = prod - jnp.mean(prod, axis=0, keepdims=True)
    hidden_scale = lax.rsqrt(jnp.mean(away * away, axis=0, keepdims=True) + EPSILON)
    hn = away * hidden_scale
    gh_away = ghid[...]
    second = jnp.mean((gh_away) * hn, axis=0, keepdims=True)
    gprod = hidden_scale * (gh_away - hn * second)
    send_gradient(gprod)

    po = dot(wo_ref[...], hn.astype(BF16), ((0,), (0,)))
    gv = gate[...]
    glogit[...] = (cot[...] * po * gv * (1.0 - gv)).astype(BF16)
    upd_ref[...] = cells_last(gv * po)

    @pl.when(is_owner)
    def _():
        gather_gradient(2)
        multiply(2, 1, ((1,), (0,)), 0)
        give_back(GRAD_LEFT, 0)
        multiply(2, 0, ((0,), (0,)), 1)
        give_back(GRAD_RIGHT, 1)

    base = dot(wg_ref[...], glogit[...], ((1,), (0,)))

    def through(base, part, back):
        masked = back * mask
        sig = proj[part]
        val = proj[part + 1]
        to_sig = (masked * val * sig * (1.0 - sig)).astype(BF16)
        to_val = (masked * sig).astype(BF16)
        base = base + dot(wp_ref[:, pl.ds(part * hidden, hidden)], to_sig, ((1,), (0,)))
        return base + dot(wp_ref[:, pl.ds((part + 1) * hidden, hidden)], to_val, ((1,), (0,)))

    pass_on(GRAD_LEFT)
    pass_on(GRAD_RIGHT)
    base = through(base, 0, arrive(GRAD_LEFT))
    base = through(base, 2, arrive(GRAD_RIGHT))

    nt = normed[...]
    first = jnp.mean(base, axis=0, keepdims=True)
    second = jnp.mean(base * nt, axis=0, keepdims=True)
    gpair_ref[...] = cells_last(pair_scale * (base - first - nt * second))

    def sent(ref, count, sem):
        some = ref.at[pl.ds(0, count)]
        push(some, some, sem, {"dap": me_d}).wait_send()

    inward = (LEFT, RIGHT)
    outward = (GRAD_LEFT, GRAD_RIGHT)
    for n in inward + outward:
        if n in BY_Z:
            sent(z_out.at[n], nz - 1, 8 * n)
        else:
            sent(ch_out.at[n], ns - 1, 8 * n)

    @pl.when(is_owner)
    def _():
        sent(own_tiles.at[0], nd * ns - 1, 8 * PRODUCT)
        sent(cell_tiles.at[1], ns * nz - 1, 8 * GRAD)
        for n in inward:
            if n in BY_Z:
                sent(col_out.at[n], ns - 1, 8 * n + 1)
            else:
                sent(row_out.at[n], nz - 1, 8 * n + 1)
        for c, n in enumerate(outward):
            if n in BY_Z:
                sent(own_cells.at[n], 4 * ns - 1, 8 * n + 1)
            else:
                sent(own_out.at[c], nd - 1, 8 * n + 1)

    @pl.when(jnp.logical_not(is_owner))
    def _():
        sent(cell_tiles.at[1], ns * nz, 8 * GRAD)
        for n in inward:
            if n in BY_Z:
                sent(col_out.at[n], ns, 8 * n + 1)
            else:
                sent(row_out.at[n], nz, 8 * n + 1)


def to_hbm(upd, gpair, upd_hbm, gpair_hbm, sem):
    copies = [
        pltpu.make_async_copy(upd, upd_hbm, sem.at[0]),
        pltpu.make_async_copy(gpair, gpair_hbm, sem.at[1]),
    ]
    for copy in copies:
        copy.start()
    for copy in copies:
        copy.wait()


def on_device(nd, ns, pair_rep, residue_mask, w_proj, w_gate, w_out, cotangent):
    hidden, chans = w_out.shape
    vmem = pl.BlockSpec(memory_space=pltpu.VMEM)
    hbm = pl.BlockSpec(memory_space=pltpu.HBM)
    shape = jax.ShapeDtypeStruct(pair_rep.shape, BF16)
    width = ns * 32
    nz = nd // 4
    args = (pair_rep, cotangent, residue_mask[None, :], w_proj, w_gate, w_out)
    args = [pltpu.with_memory_space_constraint(a, pltpu.HBM) for a in args]
    results = pl.pallas_call(
        functools.partial(kernel, nd, ns),
        out_shape=(shape, shape),
        in_specs=[hbm] * 6,
        out_specs=(vmem, vmem),
        scratch_shapes=[pltpu.VMEM(a.shape, a.dtype) for a in args]
        + [
            pltpu.VMEM((2, 16, 32, chans), BF16),
            pltpu.VMEM((8, nd * 16), F32),
            pltpu.VMEM((4, hidden, CELLS), F32),
            pltpu.VMEM((chans, CELLS), F32),
            pltpu.VMEM((chans, CELLS), F32),
            pltpu.VMEM((chans, CELLS), F32),
            pltpu.VMEM((hidden, CELLS), F32),
            pltpu.VMEM((chans, CELLS), BF16),
            pltpu.VMEM((QUADS, 16 * nz, 128), F32),
            pltpu.VMEM((6, ns, nz, CELLS), BF16),
            pltpu.VMEM((6, ns, nz, CELLS), BF16),
            pltpu.VMEM((6, nz, 16, width), BF16),
            pltpu.VMEM((6, nz, 16, width), BF16),
            pltpu.VMEM((3, nd, 16, width), BF16),
            pltpu.VMEM((3, nd, 16, width), BF16),
            pltpu.VMEM((6, nz, ns, CELLS), BF16),
            pltpu.VMEM((6, nz, ns, CELLS), BF16),
            pltpu.VMEM((6, ns, nz, CELLS), BF16),
            pltpu.VMEM((6, ns, nz, CELLS), BF16),
            pltpu.VMEM((6, 4 * ns, nz, CELLS), BF16),
            pltpu.VMEM((2, ns * nz, QUADS, 128), BF16),
            pltpu.VMEM((2, nd * ns, QUADS, 128), BF16),
            pltpu.VMEM((ns // 4, nd * 16, 128), F32),
            pltpu.VMEM((QUADS * ns * nz, 128), F32),
            pltpu.SemaphoreType.DMA((6,)),
            pltpu.SemaphoreType.DMA((48,)),
            pltpu.SemaphoreType.DMA((48,)),
        ],
        compiler_params=pltpu.CompilerParams(
            collective_id=0, has_side_effects=True, vmem_limit_bytes=50331648
        ),
    )(*args)
    return pl.pallas_call(
        to_hbm,
        out_shape=(shape, shape),
        in_specs=[vmem, vmem],
        out_specs=(hbm, hbm),
        scratch_shapes=[pltpu.SemaphoreType.DMA((2,))],
        compiler_params=pltpu.CompilerParams(vmem_limit_bytes=1024 * 1024),
    )(*results)


def solution(mesh):
    nd, ns = mesh.shape["dap"], mesh.shape["ch"]
    return jax.shard_map(
        functools.partial(on_device, nd, ns),
        mesh=mesh,
        in_specs=(P("dap", "ch", None), P(), P(), P(), P(), P("dap", "ch", None)),
        out_specs=(P("dap", "ch", None), P("dap", "ch", None)),
        check_vma=False,
    )
```

```python
import functools

import jax
import jax.numpy as jnp
from jax import lax
from jax.experimental import pallas as pl
from jax.experimental.pallas import tpu as pltpu
from jax.sharding import PartitionSpec as P

EPSILON = 1e-05
F32 = jnp.float32
BF16 = jnp.bfloat16
CELLS = 512
QUADS = CELLS // 128
LEFT, RIGHT, PRODUCT, GRAD, GRADS = range(5)
ARRIVALS = 40
BY_Z = (RIGHT,)


def ring_order(size):
    return sorted(range(size), key=lambda r: -min(r, size - r))


def ch_peers(me, ch_size):
    ny = ch_size // 2
    steps = [(dy, dx) for dy in range(ny) for dx in range(2) if dy or dx]
    steps.sort(key=lambda p: -(min(p[0], ny - p[0]) + 2 * p[1]))
    y, x = me // 2, lax.rem(me, 2)
    return [2 * lax.rem(y + dy, ny) + lax.rem(x + dx, 2) for dy, dx in steps]


def dot(a, b, contract):
    return lax.dot_general(a, b, (contract, ((), ())), preferred_element_type=F32)


def swap_blocks(rows):
    block = lax.broadcasted_iota(jnp.int32, rows[0].shape, 1) // 32
    odd = lax.rem(block, 2) == 1
    high = block >= 2
    x0, x1, x2, x3 = rows
    z0 = jnp.where(odd, pltpu.roll(x1, 32, 1), x0)
    z1 = jnp.where(odd, x1, pltpu.roll(x0, 96, 1))
    z2 = jnp.where(odd, pltpu.roll(x3, 32, 1), x2)
    z3 = jnp.where(odd, x3, pltpu.roll(x2, 96, 1))
    return (
        jnp.where(high, pltpu.roll(z2, 64, 1), z0),
        jnp.where(high, pltpu.roll(z3, 64, 1), z1),
        jnp.where(high, z2, pltpu.roll(z0, 64, 1)),
        jnp.where(high, z3, pltpu.roll(z1, 64, 1)),
    )


def cells_to_rows(cells, first, count, mid, rows, place):
    group = cells.shape[1]
    for t in range(count // 4):
        for q in range(QUADS):
            lanes = pl.ds(q * 128, 128)
            moved = swap_blocks([cells[first + 4 * t + a, :, lanes].astype(F32) for a in range(4)])
            for b in range(4):
                mid[t, pl.ds(4 * q + b, group, stride=16), :] = moved[b]
    for t in range(count // 4):
        for m in range(group):
            rows[place(m), :, pl.ds(t * 128, 128)] = mid[t, pl.ds(16 * m, 16), :].astype(BF16)


def swap_leading(src, mid, dst):
    na, nb = src.shape[0], src.shape[1]
    for q in range(QUADS):
        lanes = pl.ds(q * 128, 128)
        for a in range(na):
            mid[q, pl.ds(a * nb, nb), :] = src[a, :, lanes].astype(F32)
        for b in range(nb):
            dst[b, :, lanes] = mid[q, pl.ds(b, na, stride=nb), :].astype(BF16)


def kernel(
    nd,
    ns,
    x_hbm,
    cot_hbm,
    mask_hbm,
    wp_hbm,
    wg_hbm,
    wo_hbm,
    upd_ref,
    gpair_ref,
    x_ref,
    cot_ref,
    mask_ref,
    wp_ref,
    wg_ref,
    wo_ref,
    padded,
    live,
    proj,
    normed,
    gate,
    cot,
    ghid,
    glogit,
    mid,
    ch_out,
    ch_in,
    row_out,
    own_in,
    z_out,
    z_in,
    col_out,
    own_cells,
    prod_cell,
    prod_own,
    grad_cell,
    grad_own,
    grads_cell,
    grads_own,
    own_mid,
    flat,
    load_sem,
    send_sem,
    recv_sem,
):
    rows, columns, chans = x_ref.shape
    half = columns // 2
    nz = nd // 4
    hidden = ns * nz
    me_d = lax.axis_index("dap")
    me_s = lax.axis_index("ch")
    my_x, my_z, my_core = me_d // (2 * nz), lax.rem(me_d // 2, nz), lax.rem(me_d, 2)
    is_owner = jnp.logical_and(my_core == 1, my_x == lax.rem(my_z + me_s // 2, 2))

    def at_dap(x, z, core):
        return 2 * nz * x + 2 * z + core

    def owner_of(z, s):
        return at_dap(lax.rem(z + s // 2, 2), z, 1)

    near_ch = ch_peers(me_s, ns)
    z_order = [lax.rem(my_z + r, nz) for r in ring_order(nz)]
    other_x = 1 - my_x
    dap_order = [
        at_dap(x, z, core)
        for z in z_order
        for x in (other_x, my_x)
        for core in (0, 1)
    ][:-1]
    quarters = [(other_x, 0), (other_x, 1), (my_x, 0), (my_x, 1)]

    loads = [
        pltpu.make_async_copy(src, dst, load_sem.at[n])
        for n, (src, dst) in enumerate(
            (
                (x_hbm, x_ref),
                (wp_hbm, wp_ref),
                (mask_hbm, mask_ref),
                (cot_hbm, cot_ref),
                (wg_hbm, wg_ref),
                (wo_hbm, wo_ref),
            )
        )
    ]
    for load in loads:
        load.start()

    barrier = pltpu.get_barrier_semaphore()

    def greet(peer):
        pl.semaphore_signal(
            barrier, inc=1, device_id=peer, device_id_type=pl.DeviceIdType.MESH
        )

    for s in near_ch:
        greet({"ch": s})
    for z in z_order[:-1]:
        greet({"dap": at_dap(my_x, z, my_core)})

    @pl.when(is_owner)
    def _():
        for d in dap_order:
            greet({"dap": d})
        for x, core in quarters:
            for s in near_ch:
                greet({"dap": at_dap(x, my_z, core), "ch": s})
        for x, core in quarters[:-1]:
            greet({"dap": at_dap(x, my_z, core), "ch": me_s})

    @pl.when(jnp.logical_not(is_owner))
    def _():
        for z in z_order:
            greet({"dap": owner_of(z, me_s)})
        for s in near_ch + [me_s]:
            greet({"dap": owner_of(my_z, s), "ch": s})

    greetings = (
        ns - 1 + nz - 1 + jnp.where(is_owner, nd - 1 + 4 * ns - 1, nz + ns)
    )

    def push(src, dst, sem, peer, arrival=None):
        return pltpu.make_async_remote_copy(
            src_ref=src,
            dst_ref=dst,
            send_sem=send_sem.at[sem],
            recv_sem=recv_sem.at[sem if arrival is None else arrival],
            device_id=peer,
            device_id_type=pl.DeviceIdType.MESH,
        )

    def await_slabs(ref, count, sem):
        some = ref.at[pl.ds(0, count)]
        push(some, some, sem, {"dap": me_d}).wait_recv()

    def await_all_but_mine(ref, sem):
        @pl.when(is_owner)
        def _():
            await_slabs(ref, ref.shape[0] - 1, sem)

        @pl.when(jnp.logical_not(is_owner))
        def _():
            await_slabs(ref, ref.shape[0], sem)

    def across_ch(n):
        src, dst, sem = ch_out.at[n], ch_in.at[n], 8 * n
        for s in near_ch:
            push(src.at[s], dst.at[me_s], sem, {"ch": s}).start()
        dst[me_s] = src[me_s]

    def across_z(n):
        src, dst, sem = z_out.at[n], z_in.at[n], 8 * n
        for z in z_order[:-1]:
            push(src.at[z], dst.at[my_z], sem, {"dap": at_dap(my_x, z, my_core)}).start()
        dst[my_z] = src[my_z]

    def rows_to_owners(n, a):
        src, dst, sem = row_out.at[n], own_in.at[a], 8 * n + 1

        def send(z):
            push(src.at[z], dst.at[me_d], sem, {"dap": owner_of(z, me_s)}).start()

        for z in z_order[:-1]:
            send(z)

        @pl.when(is_owner)
        def _():
            dst[me_d] = src[my_z]

        @pl.when(jnp.logical_not(is_owner))
        def _():
            send(my_z)

    def columns_to_owners(n):
        quarter = 2 * my_x + my_core
        slot = quarter * ns + me_s
        sem = 8 * n + 1

        def send(s):
            peer = {"dap": owner_of(my_z, s), "ch": s}
            push(col_out.at[n, s], own_cells.at[n, slot], sem, peer, sem + quarter).start()

        for s in near_ch:
            send(s)

        @pl.when(is_owner)
        def _():
            own_cells[n, slot] = col_out[n, me_s]

        @pl.when(jnp.logical_not(is_owner))
        def _():
            send(me_s)

    def leave(n, value):
        if n in BY_Z:
            for q in range(QUADS):
                lanes = slice(q * 128, q * 128 + 128)
                mid[q, 0:hidden, :] = value[:, lanes]
                for z in range(nz):
                    z_out[n, z, :, lanes] = mid[q, pl.ds(z, ns, stride=nz), :].astype(BF16)
        else:
            ch_out[n] = value.reshape(ns, nz, CELLS).astype(BF16)

    def across(n):
        if n in BY_Z:
            across_z(n)
        else:
            across_ch(n)

    def forward(n, a):
        if n in BY_Z:
            await_slabs(z_in.at[n], nz - 1, 8 * n)
            swap_leading(z_in.at[n], mid, col_out.at[n])
            columns_to_owners(n)
        else:
            await_slabs(ch_in.at[n], ns - 1, 8 * n)
            cells_to_rows(ch_in.at[n], 0, ns, mid, row_out.at[n], lambda m: m)
            rows_to_owners(n, a)

    def gathered(n, a):
        if n not in BY_Z:
            await_slabs(own_in.at[a], nd - 1, 8 * n + 1)
            return

        def arrived(x, core, count):
            quarter = 2 * x + core
            await_slabs(own_cells.at[n], count, 8 * n + 1 + quarter)
            cells_to_rows(
                own_cells.at[n],
                quarter * ns,
                ns,
                mid,
                own_in.at[a],
                lambda z: at_dap(x, z, core),
            )

        arrived(my_x, 1, ns - 1)

        @pl.loop(0, 3)
        def _(r):
            arrived(jnp.where(r == 0, my_x, other_x), lax.rem(r, 2), ns)

    width = ns * 32
    many = nd * 16
    tiles = ns // 4

    def multiply(a, b, contract, k, h):
        right = own_in[b].reshape(many, width)
        if contract[0][0] == 1:
            part = own_in[a, pl.ds(h * nd // 2, nd // 2)].reshape(many // 2, width)
        else:
            part = own_in[a, :, :, pl.ds(h * width // 2, width // 2)].reshape(many, width // 2)
        value = dot(part, right, contract)
        for t in range(tiles):
            own_mid[k, t, pl.ds(h * many // 2, many // 2), :] = value[:, t * 128 : t * 128 + 128]

    my_tile = me_s // 4
    me = me_d * ns + me_s

    def tile_at(step):
        shift = jnp.where(lax.rem(step, 2) == 1, -((step + 1) // 2), step // 2)
        return lax.rem(my_tile + tiles // 2 + shift, tiles)

    def tiles_back(own, cell, sem, h, kinds, whole):
        mine = me_s * nz + my_z

        @pl.loop(0, tiles)
        def _(step):
            t = tile_at(step)
            for k in kinds:
                for p in range(h * nz, h * nz + nz):
                    moved = swap_blocks(
                        [own_mid[k, t, pl.ds(32 * p + b, 8, stride=4), :] for b in range(4)]
                    )
                    for a in range(4):
                        line = moved[a].astype(BF16)
                        for core in range(2):
                            own[(2 * p + core) * ns + 4 * t + a, k] = line[4 * core : 4 * core + 4]
            for n, z in enumerate(z_order):
                for core in range(2):
                    d = at_dap(h, z, core)
                    for a in range(4):
                        s = 4 * t + a

                        def send(d=d, s=s):
                            src, dst = own.at[d * ns + s], cell.at[mine]
                            if not whole:
                                src, dst = src.at[kinds[0]], dst.at[kinds[0]]
                            push(src, dst, sem, {"dap": d, "ch": s}).start()

                        if n == nz - 1 and core == 1:
                            pl.when(d * ns + s != me)(send)
                        else:
                            send()

    def tiles_at_cells(cell, sem):
        await_all_but_mine(cell, sem)
        found = []
        for k in range(cell.shape[1]):
            for c in range(hidden):
                flat[pl.ds(4 * c, 4), :] = cell[c, k].astype(F32)
            found.append(
                jnp.concatenate(
                    [flat[pl.ds(q, hidden, stride=QUADS), :] for q in range(QUADS)], axis=1
                )
            )
        return found

    def tiles_to_owners(value):
        n = GRAD
        for q in range(QUADS):
            flat[pl.ds(q, hidden, stride=QUADS), :] = value[:, q * 128 : q * 128 + 128]
        for c in range(hidden // 2):
            pair = flat[pl.ds(8 * c, 8), :].astype(BF16)
            grad_cell[2 * c] = pair[0:4]
            grad_cell[2 * c + 1] = pair[4:8]

        ny = ns // 2
        steps = [(dz, dy, dx) for dz in range(nz) for dy in range(ny) for dx in range(2)]
        steps.sort(key=lambda p: -(min(p[0], nz - p[0]) + min(p[1], ny - p[1]) + 2 * p[2]))
        for dz, dy, dx in steps:
            z = lax.rem(my_z + dz, nz)
            s = 2 * lax.rem(me_s // 2 + dy, ny) + lax.rem(me_s + dx, 2)

            def send(z=z, s=s):
                push(
                    grad_cell.at[s * nz + z],
                    grad_own.at[me],
                    8 * n,
                    {"dap": owner_of(z, s), "ch": s},
                    ARRIVALS + 4 * my_x + my_tile,
                ).start()

            if dz or dy or dx:
                send()
            else:
                pl.when(jnp.logical_not(is_owner))(send)

        @pl.when(is_owner)
        def _():
            grad_own[me] = grad_cell[me_s * nz + my_z]

    def tiles_gathered(a, h):
        @pl.loop(0, tiles)
        def _(step):
            t = tile_at(tiles - 1 - step)

            def arrived(count):
                some = grad_own.at[pl.ds(0, count)]
                push(some, some, 8 * GRAD, {"dap": me_d}, ARRIVALS + 4 * h + t).wait_recv()

            mine_too = jnp.logical_and(t == my_tile, my_x == h)
            pl.when(mine_too)(lambda: arrived(2 * nd - 1))
            pl.when(jnp.logical_not(mine_too))(lambda: arrived(2 * nd))
            for p in range(h * nz, h * nz + nz):
                got = [
                    jnp.concatenate(
                        [
                            grad_own[(2 * p + core) * ns + 4 * t + e].astype(F32)
                            for core in range(2)
                        ],
                        axis=0,
                    )
                    for e in range(4)
                ]
                for b, rows in enumerate(swap_blocks(got)):
                    own_mid[0, t, pl.ds(32 * p + b, 8, stride=4), :] = rows
            lanes = pl.ds(pl.multiple_of(t * 128, 128), 128)
            for d in range(h * nd // 2, (h + 1) * nd // 2):
                own_in[a, d, :, lanes] = own_mid[0, t, pl.ds(16 * d, 16), :].astype(BF16)

    lane = lax.broadcasted_iota(jnp.int32, (1, CELLS), 1)
    place = lax.rem(lane, 16)
    used = jnp.logical_and(place < half, lane < rows * 32)
    first_half = lax.rem(lane, 32) < 16

    eye = (
        lax.broadcasted_iota(jnp.int32, (chans, chans), 0)
        == lax.broadcasted_iota(jnp.int32, (chans, chans), 1)
    ).astype(F32).astype(BF16)

    def cells_first(ref, slot):
        padded[slot] = jnp.zeros(padded.shape[1:], BF16)
        padded[slot, 0:rows, 0:columns, :] = ref[...]
        flat = padded[slot].reshape(CELLS, chans)
        turned = dot(eye, flat, ((1,), (1,)))
        spread = jnp.where(first_half, turned, pltpu.roll(turned, 1, 1))
        return jnp.where(used, spread, 0.0)

    def cells_last(turned):
        closed = jnp.where(
            lax.rem(lane, 32) < half, turned, pltpu.roll(turned, CELLS - 1, 1)
        )
        return closed.T.reshape(16, 32, chans)[0:rows, 0:columns, :].astype(BF16)

    residues = mask_ref.shape[1]
    total = nd * 16
    loads[2].wait()
    live[...] = jnp.zeros(live.shape, F32)
    live[:, 0:residues] = jnp.broadcast_to(mask_ref[...].astype(F32), (8, residues))
    flags = live[...].astype(BF16)

    def one_hot(hot):
        return jnp.where(hot, 1.0, 0.0).astype(BF16)

    at = lax.broadcasted_iota(jnp.int32, (total, 128), 0)
    lane_1 = lax.broadcasted_iota(jnp.int32, (total, 128), 1)
    row_flags = dot(
        flags, one_hot(jnp.logical_and(at == rows * me_d + lane_1, lane_1 < rows)), ((1,), (0,))
    )
    col_at = columns * me_s + half * (lax.rem(lane_1, 32) // 16) + lax.rem(lane_1, 16)
    col_flags = dot(
        flags, one_hot(jnp.logical_and(at == col_at, lax.rem(lane_1, 16) < half)), ((1,), (0,))
    )
    spot = lax.broadcasted_iota(jnp.int32, (128, CELLS), 0)
    row_of = lax.broadcasted_iota(jnp.int32, (128, CELLS), 1) // 32
    row_mask = dot(row_flags.astype(BF16), one_hot(spot == row_of), ((1,), (0,)))
    col_mask = jnp.concatenate([col_flags] * (CELLS // 128), axis=1)
    mask = (row_mask * col_mask)[0:1]

    loads[0].wait()
    xt = cells_first(x_ref, 0)
    center = jnp.mean(xt, axis=0, keepdims=True)
    spread = xt - center
    pair_scale = lax.rsqrt(jnp.mean(spread * spread, axis=0, keepdims=True) + EPSILON)
    nt = spread * pair_scale
    normed[...] = nt
    nh = nt.astype(BF16)

    def project(part):
        raw = dot(wp_ref[:, pl.ds(part * hidden, hidden)], nh, ((0,), (0,)))
        return raw

    def edge(part):
        sig = jax.nn.sigmoid(project(part))
        val = project(part + 1)
        proj[part] = sig
        proj[part + 1] = val
        return sig * val * mask

    loads[1].wait()
    leave(LEFT, edge(0))
    leave(RIGHT, edge(2))
    pl.semaphore_wait(barrier, greetings)
    across(RIGHT)
    across(LEFT)

    for load in loads[3:]:
        load.wait()
    gv = jax.nn.sigmoid(dot(wg_ref[...], nh, ((0,), (0,))))
    gate[...] = gv
    ct = cells_first(cot_ref, 1)
    cot[...] = ct
    gh = dot(wo_ref[...], (ct * gv).astype(BF16), ((1,), (0,)))
    ghid[...] = gh - jnp.mean(gh, axis=0, keepdims=True)

    forward(RIGHT, 1)
    forward(LEFT, 0)

    @pl.when(is_owner)
    def _():
        gathered(RIGHT, 1)
        gathered(LEFT, 0)
        for h in range(2):
            multiply(0, 1, ((1,), (1,)), 0, h)
            tiles_back(prod_own, prod_cell, 8 * PRODUCT, h, (0,), True)
        prod_cell[me_s * nz + my_z] = prod_own[me]

    (prod,) = tiles_at_cells(prod_cell, 8 * PRODUCT)
    away = prod - jnp.mean(prod, axis=0, keepdims=True)
    hidden_scale = lax.rsqrt(jnp.mean(away * away, axis=0, keepdims=True) + EPSILON)
    hn = away * hidden_scale
    gh_away = ghid[...]
    second = jnp.mean((gh_away) * hn, axis=0, keepdims=True)
    gprod = hidden_scale * (gh_away - hn * second)
    tiles_to_owners(gprod)

    po = dot(wo_ref[...], hn.astype(BF16), ((0,), (0,)))
    gv = gate[...]
    glogit[...] = (cot[...] * po * gv * (1.0 - gv)).astype(BF16)
    upd_ref[...] = cells_last(gv * po)

    @pl.when(is_owner)
    def _():
        tiles_gathered(2, 0)
        multiply(2, 1, ((1,), (0,)), 0, 0)
        tiles_back(grads_own, grads_cell, 8 * GRADS, 0, (0,), False)
        tiles_gathered(2, 1)
        multiply(2, 1, ((1,), (0,)), 0, 1)
        multiply(2, 0, ((0,), (0,)), 1, 1)
        tiles_back(grads_own, grads_cell, 8 * GRADS, 1, (0, 1), True)
        multiply(2, 0, ((0,), (0,)), 1, 0)
        tiles_back(grads_own, grads_cell, 8 * GRADS, 0, (1,), False)
        grads_cell[me_s * nz + my_z] = grads_own[me]

    base = dot(wg_ref[...], glogit[...], ((1,), (0,)))

    def through(base, part, back):
        masked = back * mask
        sig = proj[part]
        val = proj[part + 1]
        to_sig = (masked * val * sig * (1.0 - sig)).astype(BF16)
        to_val = (masked * sig).astype(BF16)
        base = base + dot(wp_ref[:, pl.ds(part * hidden, hidden)], to_sig, ((1,), (0,)))
        return base + dot(wp_ref[:, pl.ds((part + 1) * hidden, hidden)], to_val, ((1,), (0,)))

    back_left, back_right = tiles_at_cells(grads_cell, 8 * GRADS)
    base = through(base, 0, back_left)
    base = through(base, 2, back_right)

    nt = normed[...]
    first = jnp.mean(base, axis=0, keepdims=True)
    second = jnp.mean(base * nt, axis=0, keepdims=True)
    gpair_ref[...] = cells_last(pair_scale * (base - first - nt * second))

    def sent(ref, count, sem):
        some = ref.at[pl.ds(0, count)]
        push(some, some, sem, {"dap": me_d}).wait_send()

    sent(ch_out.at[LEFT], ns - 1, 8 * LEFT)
    sent(z_out.at[RIGHT], nz - 1, 8 * RIGHT)

    @pl.when(is_owner)
    def _():
        sent(row_out.at[LEFT], nz - 1, 8 * LEFT + 1)
        sent(col_out.at[RIGHT], ns - 1, 8 * RIGHT + 1)
        sent(grad_cell, hidden - 1, 8 * GRAD)
        sent(prod_own, nd * ns - 1, 8 * PRODUCT)
        sent(grads_own, nd * ns - 1, 8 * GRADS)

    @pl.when(jnp.logical_not(is_owner))
    def _():
        sent(row_out.at[LEFT], nz, 8 * LEFT + 1)
        sent(col_out.at[RIGHT], ns, 8 * RIGHT + 1)
        sent(grad_cell, hidden, 8 * GRAD)


def to_hbm(upd, gpair, upd_hbm, gpair_hbm, sem):
    copies = [
        pltpu.make_async_copy(upd, upd_hbm, sem.at[0]),
        pltpu.make_async_copy(gpair, gpair_hbm, sem.at[1]),
    ]
    for copy in copies:
        copy.start()
    for copy in copies:
        copy.wait()


def on_device(nd, ns, pair_rep, residue_mask, w_proj, w_gate, w_out, cotangent):
    hidden, chans = w_out.shape
    vmem = pl.BlockSpec(memory_space=pltpu.VMEM)
    hbm = pl.BlockSpec(memory_space=pltpu.HBM)
    shape = jax.ShapeDtypeStruct(pair_rep.shape, BF16)
    width = ns * 32
    nz = nd // 4
    args = (pair_rep, cotangent, residue_mask[None, :], w_proj, w_gate, w_out)
    args = [pltpu.with_memory_space_constraint(a, pltpu.HBM) for a in args]
    results = pl.pallas_call(
        functools.partial(kernel, nd, ns),
        out_shape=(shape, shape),
        in_specs=[hbm] * 6,
        out_specs=(vmem, vmem),
        scratch_shapes=[pltpu.VMEM(a.shape, a.dtype) for a in args]
        + [
            pltpu.VMEM((2, 16, 32, chans), BF16),
            pltpu.VMEM((8, nd * 16), F32),
            pltpu.VMEM((4, hidden, CELLS), F32),
            pltpu.VMEM((chans, CELLS), F32),
            pltpu.VMEM((chans, CELLS), F32),
            pltpu.VMEM((chans, CELLS), F32),
            pltpu.VMEM((hidden, CELLS), F32),
            pltpu.VMEM((chans, CELLS), BF16),
            pltpu.VMEM((QUADS, 16 * nz, 128), F32),
            pltpu.VMEM((2, ns, nz, CELLS), BF16),
            pltpu.VMEM((2, ns, nz, CELLS), BF16),
            pltpu.VMEM((2, nz, 16, width), BF16),
            pltpu.VMEM((3, nd, 16, width), BF16),
            pltpu.VMEM((2, nz, ns, CELLS), BF16),
            pltpu.VMEM((2, nz, ns, CELLS), BF16),
            pltpu.VMEM((2, ns, nz, CELLS), BF16),
            pltpu.VMEM((2, 4 * ns, nz, CELLS), BF16),
            pltpu.VMEM((ns * nz, 1, QUADS, 128), BF16),
            pltpu.VMEM((nd * ns, 1, QUADS, 128), BF16),
            pltpu.VMEM((ns * nz, QUADS, 128), BF16),
            pltpu.VMEM((nd * ns, QUADS, 128), BF16),
            pltpu.VMEM((ns * nz, 2, QUADS, 128), BF16),
            pltpu.VMEM((nd * ns, 2, QUADS, 128), BF16),
            pltpu.VMEM((2, ns // 4, nd * 16, 128), F32),
            pltpu.VMEM((QUADS * ns * nz, 128), F32),
            pltpu.SemaphoreType.DMA((6,)),
            pltpu.SemaphoreType.DMA((48,)),
            pltpu.SemaphoreType.DMA((48,)),
        ],
        compiler_params=pltpu.CompilerParams(
            collective_id=0, has_side_effects=True, vmem_limit_bytes=50331648
        ),
    )(*args)
    return pl.pallas_call(
        to_hbm,
        out_shape=(shape, shape),
        in_specs=[vmem, vmem],
        out_specs=(hbm, hbm),
        scratch_shapes=[pltpu.SemaphoreType.DMA((2,))],
        compiler_params=pltpu.CompilerParams(vmem_limit_bytes=1024 * 1024),
    )(*results)


def solution(mesh):
    nd, ns = mesh.shape["dap"], mesh.shape["ch"]
    return jax.shard_map(
        functools.partial(on_device, nd, ns),
        mesh=mesh,
        in_specs=(P("dap", "ch", None), P(), P(), P(), P(), P("dap", "ch", None)),
        out_specs=(P("dap", "ch", None), P("dap", "ch", None)),
        check_vma=False,
    )
```

```python
import functools

import jax
import jax.numpy as jnp
from jax import lax
from jax.experimental import pallas as pl
from jax.experimental.pallas import tpu as pltpu
from jax.sharding import PartitionSpec as P

EPSILON = 1e-05
F32 = jnp.float32
BF16 = jnp.bfloat16
CELLS = 512
QUADS = CELLS // 128
LEFT, RIGHT, PRODUCT, GRAD, GRADS = range(5)
ARRIVALS = 40
BY_Z = (RIGHT,)


def ring_order(size):
    return sorted(range(size), key=lambda r: -min(r, size - r))


def ch_peers(me, ch_size):
    ny = ch_size // 2
    steps = [(dy, dx) for dy in range(ny) for dx in range(2) if dy or dx]
    steps.sort(key=lambda p: -(min(p[0], ny - p[0]) + 2 * p[1]))
    y, x = me // 2, lax.rem(me, 2)
    return [2 * lax.rem(y + dy, ny) + lax.rem(x + dx, 2) for dy, dx in steps]


def dot(a, b, contract):
    return lax.dot_general(a, b, (contract, ((), ())), preferred_element_type=F32)


def swap_blocks(rows):
    block = lax.broadcasted_iota(jnp.int32, rows[0].shape, 1) // 32
    odd = lax.rem(block, 2) == 1
    high = block >= 2
    x0, x1, x2, x3 = rows
    z0 = jnp.where(odd, pltpu.roll(x1, 32, 1), x0)
    z1 = jnp.where(odd, x1, pltpu.roll(x0, 96, 1))
    z2 = jnp.where(odd, pltpu.roll(x3, 32, 1), x2)
    z3 = jnp.where(odd, x3, pltpu.roll(x2, 96, 1))
    return (
        jnp.where(high, pltpu.roll(z2, 64, 1), z0),
        jnp.where(high, pltpu.roll(z3, 64, 1), z1),
        jnp.where(high, z2, pltpu.roll(z0, 64, 1)),
        jnp.where(high, z3, pltpu.roll(z1, 64, 1)),
    )


def cells_to_rows(cells, first, count, mid, rows, place):
    group = cells.shape[1]
    for t in range(count // 4):
        for q in range(QUADS):
            lanes = pl.ds(q * 128, 128)
            moved = swap_blocks([cells[first + 4 * t + a, :, lanes].astype(F32) for a in range(4)])
            for b in range(4):
                mid[t, pl.ds(4 * q + b, group, stride=16), :] = moved[b]
    for t in range(count // 4):
        for m in range(group):
            rows[place(m), :, pl.ds(t * 128, 128)] = mid[t, pl.ds(16 * m, 16), :].astype(BF16)


def swap_leading(src, mid, dst):
    na, nb = src.shape[0], src.shape[1]
    for q in range(QUADS):
        lanes = pl.ds(q * 128, 128)
        for a in range(na):
            mid[q, pl.ds(a * nb, nb), :] = src[a, :, lanes].astype(F32)
        for b in range(nb):
            dst[b, :, lanes] = mid[q, pl.ds(b, na, stride=nb), :].astype(BF16)


def kernel(
    nd,
    ns,
    x_hbm,
    cot_hbm,
    mask_hbm,
    wp_hbm,
    wg_hbm,
    wo_hbm,
    upd_ref,
    gpair_ref,
    x_ref,
    cot_ref,
    mask_ref,
    wp_ref,
    wg_ref,
    wo_ref,
    padded,
    live,
    proj,
    normed,
    gate,
    cot,
    ghid,
    glogit,
    mid,
    ch_out,
    ch_in,
    row_out,
    own_in,
    z_out,
    z_in,
    col_out,
    own_cells,
    prod_cell,
    prod_own,
    grad_cell,
    grad_own,
    grads_cell,
    grads_own,
    own_mid,
    flat,
    load_sem,
    send_sem,
    recv_sem,
):
    rows, columns, chans = x_ref.shape
    half = columns // 2
    nz = nd // 4
    hidden = ns * nz
    me_d = lax.axis_index("dap")
    me_s = lax.axis_index("ch")
    my_x, my_z, my_core = me_d // (2 * nz), lax.rem(me_d // 2, nz), lax.rem(me_d, 2)
    is_owner = jnp.logical_and(my_core == 1, my_x == lax.rem(my_z + me_s // 2, 2))

    def at_dap(x, z, core):
        return 2 * nz * x + 2 * z + core

    def owner_of(z, s):
        return at_dap(lax.rem(z + s // 2, 2), z, 1)

    near_ch = ch_peers(me_s, ns)
    z_order = [lax.rem(my_z + r, nz) for r in ring_order(nz)]
    other_x = 1 - my_x
    dap_order = [
        at_dap(x, z, core)
        for z in z_order
        for x in (other_x, my_x)
        for core in (0, 1)
    ][:-1]
    quarters = [(other_x, 0), (other_x, 1), (my_x, 0), (my_x, 1)]

    loads = [
        pltpu.make_async_copy(src, dst, load_sem.at[n])
        for n, (src, dst) in enumerate(
            (
                (x_hbm, x_ref),
                (wp_hbm, wp_ref),
                (mask_hbm, mask_ref),
                (cot_hbm, cot_ref),
                (wg_hbm, wg_ref),
                (wo_hbm, wo_ref),
            )
        )
    ]
    for load in loads:
        load.start()

    barrier = pltpu.get_barrier_semaphore()

    def greet(peer):
        pl.semaphore_signal(
            barrier, inc=1, device_id=peer, device_id_type=pl.DeviceIdType.MESH
        )

    for s in near_ch:
        greet({"ch": s})
    for z in z_order[:-1]:
        greet({"dap": at_dap(my_x, z, my_core)})

    @pl.when(is_owner)
    def _():
        for d in dap_order:
            greet({"dap": d})
        for x, core in quarters:
            for s in near_ch:
                greet({"dap": at_dap(x, my_z, core), "ch": s})
        for x, core in quarters[:-1]:
            greet({"dap": at_dap(x, my_z, core), "ch": me_s})

    @pl.when(jnp.logical_not(is_owner))
    def _():
        for z in z_order:
            greet({"dap": owner_of(z, me_s)})
        for s in near_ch + [me_s]:
            greet({"dap": owner_of(my_z, s), "ch": s})

    greetings = (
        ns - 1 + nz - 1 + jnp.where(is_owner, nd - 1 + 4 * ns - 1, nz + ns)
    )

    def push(src, dst, sem, peer, arrival=None):
        return pltpu.make_async_remote_copy(
            src_ref=src,
            dst_ref=dst,
            send_sem=send_sem.at[sem],
            recv_sem=recv_sem.at[sem if arrival is None else arrival],
            device_id=peer,
            device_id_type=pl.DeviceIdType.MESH,
        )

    def await_slabs(ref, count, sem):
        some = ref.at[pl.ds(0, count)]
        push(some, some, sem, {"dap": me_d}).wait_recv()

    def await_all_but_mine(ref, sem):
        @pl.when(is_owner)
        def _():
            await_slabs(ref, ref.shape[0] - 1, sem)

        @pl.when(jnp.logical_not(is_owner))
        def _():
            await_slabs(ref, ref.shape[0], sem)

    def across_ch(n):
        src, dst, sem = ch_out.at[n], ch_in.at[n], 8 * n
        for s in near_ch:
            push(src.at[s], dst.at[me_s], sem, {"ch": s}).start()
        dst[me_s] = src[me_s]

    def across_z(n):
        src, dst, sem = z_out.at[n], z_in.at[n], 8 * n
        for z in z_order[:-1]:
            push(src.at[z], dst.at[my_z], sem, {"dap": at_dap(my_x, z, my_core)}).start()
        dst[my_z] = src[my_z]

    def rows_to_owners(n, a):
        src, dst, sem = row_out.at[n], own_in.at[a], 8 * n + 1

        def send(z):
            push(src.at[z], dst.at[me_d], sem, {"dap": owner_of(z, me_s)}).start()

        for z in z_order[:-1]:
            send(z)

        @pl.when(is_owner)
        def _():
            dst[me_d] = src[my_z]

        @pl.when(jnp.logical_not(is_owner))
        def _():
            send(my_z)

    def columns_to_owners(n):
        quarter = 2 * my_x + my_core
        slot = quarter * ns + me_s
        sem = 8 * n + 1

        def send(s):
            peer = {"dap": owner_of(my_z, s), "ch": s}
            push(col_out.at[n, s], own_cells.at[n, slot], sem, peer, sem + quarter).start()

        for s in near_ch:
            send(s)

        @pl.when(is_owner)
        def _():
            own_cells[n, slot] = col_out[n, me_s]

        @pl.when(jnp.logical_not(is_owner))
        def _():
            send(me_s)

    def leave(n, value):
        if n in BY_Z:
            for q in range(QUADS):
                lanes = slice(q * 128, q * 128 + 128)
                mid[q, 0:hidden, :] = value[:, lanes]
                for z in range(nz):
                    z_out[n, z, :, lanes] = mid[q, pl.ds(z, ns, stride=nz), :].astype(BF16)
        else:
            ch_out[n] = value.reshape(ns, nz, CELLS).astype(BF16)

    def across(n):
        if n in BY_Z:
            across_z(n)
        else:
            across_ch(n)

    def forward(n, a):
        if n in BY_Z:
            await_slabs(z_in.at[n], nz - 1, 8 * n)
            swap_leading(z_in.at[n], mid, col_out.at[n])
            columns_to_owners(n)
        else:
            await_slabs(ch_in.at[n], ns - 1, 8 * n)
            cells_to_rows(ch_in.at[n], 0, ns, mid, row_out.at[n], lambda m: m)
            rows_to_owners(n, a)

    def gathered(n, a):
        if n not in BY_Z:
            await_slabs(own_in.at[a], nd - 1, 8 * n + 1)
            return

        def arrived(x, core, count):
            quarter = 2 * x + core
            await_slabs(own_cells.at[n], count, 8 * n + 1 + quarter)
            cells_to_rows(
                own_cells.at[n],
                quarter * ns,
                ns,
                mid,
                own_in.at[a],
                lambda z: at_dap(x, z, core),
            )

        arrived(my_x, 1, ns - 1)

        @pl.loop(0, 3)
        def _(r):
            arrived(jnp.where(r == 0, my_x, other_x), lax.rem(r, 2), ns)

    width = ns * 32
    many = nd * 16
    tiles = ns // 4

    hz = nz // 2
    my_half = my_z // hz
    run = 2 * hz

    def multiply(a, b, contract, k, h):
        right = own_in[b].reshape(many, width)
        for x in range(2):
            first = (2 * x + h) * run
            if contract[0][0] == 1:
                part = own_in[a, pl.ds(first, run)].reshape(16 * run, width)
            else:
                part = own_in[a, :, :, pl.ds(16 * first, 16 * run)].reshape(many, 16 * run)
            value = dot(part, right, contract)
            for t in range(tiles):
                own_mid[k, t, pl.ds(16 * first, 16 * run), :] = value[:, t * 128 : t * 128 + 128]

    my_tile = me_s // 4
    me = me_d * ns + me_s

    def tile_at(step):
        shift = jnp.where(lax.rem(step, 2) == 1, -((step + 1) // 2), step // 2)
        return lax.rem(my_tile + tiles // 2 + shift, tiles)

    def half_pairs(h):
        return [x * nz + h * hz + z for x in range(2) for z in range(hz)]

    def tiles_back(own, cell, sem, h, kinds, whole):
        mine = me_s * nz + my_z
        turn = jnp.where(my_half == h, 0, hz // 2)
        zs = [h * hz + lax.rem(my_z + r + turn, hz) for r in ring_order(hz)]
        places = [(x, z) for z in zs for x in (other_x, my_x)]

        @pl.loop(0, tiles)
        def _(step):
            t = tile_at(step)
            for k in kinds:
                for p in half_pairs(h):
                    moved = swap_blocks(
                        [own_mid[k, t, pl.ds(32 * p + b, 8, stride=4), :] for b in range(4)]
                    )
                    for a in range(4):
                        line = moved[a].astype(BF16)
                        for core in range(2):
                            own[(2 * p + core) * ns + 4 * t + a, k] = line[4 * core : 4 * core + 4]
            for n, (x, z) in enumerate(places):
                for core in range(2):
                    d = at_dap(x, z, core)
                    for a in range(4):
                        s = 4 * t + a

                        def send(d=d, s=s):
                            src, dst = own.at[d * ns + s], cell.at[mine]
                            if not whole:
                                src, dst = src.at[kinds[0]], dst.at[kinds[0]]
                            push(src, dst, sem, {"dap": d, "ch": s}).start()

                        if n == nz - 1 and core == 1:
                            pl.when(d * ns + s != me)(send)
                        else:
                            send()

    def tiles_at_cells(cell, sem):
        await_all_but_mine(cell, sem)
        found = []
        for k in range(cell.shape[1]):
            for c in range(hidden):
                flat[pl.ds(4 * c, 4), :] = cell[c, k].astype(F32)
            found.append(
                jnp.concatenate(
                    [flat[pl.ds(q, hidden, stride=QUADS), :] for q in range(QUADS)], axis=1
                )
            )
        return found

    def tiles_to_owners(value):
        n = GRAD
        for q in range(QUADS):
            flat[pl.ds(q, hidden, stride=QUADS), :] = value[:, q * 128 : q * 128 + 128]
        for c in range(hidden // 2):
            pair = flat[pl.ds(8 * c, 8), :].astype(BF16)
            grad_cell[2 * c] = pair[0:4]
            grad_cell[2 * c + 1] = pair[4:8]

        ny = ns // 2
        steps = [(dz, dy, dx) for dz in range(nz) for dy in range(ny) for dx in range(2)]
        steps.sort(key=lambda p: -(min(p[0], nz - p[0]) + min(p[1], ny - p[1]) + 2 * p[2]))
        for dz, dy, dx in steps:
            z = lax.rem(my_z + dz, nz)
            s = 2 * lax.rem(me_s // 2 + dy, ny) + lax.rem(me_s + dx, 2)

            def send(z=z, s=s):
                push(
                    grad_cell.at[s * nz + z],
                    grad_own.at[me],
                    8 * n,
                    {"dap": owner_of(z, s), "ch": s},
                    ARRIVALS + 4 * my_half + my_tile,
                ).start()

            if dz or dy or dx:
                send()
            else:
                pl.when(jnp.logical_not(is_owner))(send)

        @pl.when(is_owner)
        def _():
            grad_own[me] = grad_cell[me_s * nz + my_z]

    def tiles_gathered(a, h):
        @pl.loop(0, tiles)
        def _(step):
            t = tile_at(tiles - 1 - step)

            def arrived(count):
                some = grad_own.at[pl.ds(0, count)]
                push(some, some, 8 * GRAD, {"dap": me_d}, ARRIVALS + 4 * h + t).wait_recv()

            mine_too = jnp.logical_and(t == my_tile, my_half == h)
            pl.when(mine_too)(lambda: arrived(2 * nd - 1))
            pl.when(jnp.logical_not(mine_too))(lambda: arrived(2 * nd))
            for p in half_pairs(h):
                got = [
                    jnp.concatenate(
                        [
                            grad_own[(2 * p + core) * ns + 4 * t + e].astype(F32)
                            for core in range(2)
                        ],
                        axis=0,
                    )
                    for e in range(4)
                ]
                for b, rows in enumerate(swap_blocks(got)):
                    own_mid[0, t, pl.ds(32 * p + b, 8, stride=4), :] = rows
            lanes = pl.ds(pl.multiple_of(t * 128, 128), 128)
            for d in [2 * p + core for p in half_pairs(h) for core in range(2)]:
                own_in[a, d, :, lanes] = own_mid[0, t, pl.ds(16 * d, 16), :].astype(BF16)

    lane = lax.broadcasted_iota(jnp.int32, (1, CELLS), 1)
    place = lax.rem(lane, 16)
    used = jnp.logical_and(place < half, lane < rows * 32)
    first_half = lax.rem(lane, 32) < 16

    eye = (
        lax.broadcasted_iota(jnp.int32, (chans, chans), 0)
        == lax.broadcasted_iota(jnp.int32, (chans, chans), 1)
    ).astype(F32).astype(BF16)

    def cells_first(ref, slot):
        padded[slot] = jnp.zeros(padded.shape[1:], BF16)
        padded[slot, 0:rows, 0:columns, :] = ref[...]
        flat = padded[slot].reshape(CELLS, chans)
        turned = dot(eye, flat, ((1,), (1,)))
        spread = jnp.where(first_half, turned, pltpu.roll(turned, 1, 1))
        return jnp.where(used, spread, 0.0)

    def cells_last(turned):
        closed = jnp.where(
            lax.rem(lane, 32) < half, turned, pltpu.roll(turned, CELLS - 1, 1)
        )
        return closed.T.reshape(16, 32, chans)[0:rows, 0:columns, :].astype(BF16)

    residues = mask_ref.shape[1]
    total = nd * 16
    loads[2].wait()
    live[...] = jnp.zeros(live.shape, F32)
    live[:, 0:residues] = jnp.broadcast_to(mask_ref[...].astype(F32), (8, residues))
    flags = live[...].astype(BF16)

    def one_hot(hot):
        return jnp.where(hot, 1.0, 0.0).astype(BF16)

    at = lax.broadcasted_iota(jnp.int32, (total, 128), 0)
    lane_1 = lax.broadcasted_iota(jnp.int32, (total, 128), 1)
    row_flags = dot(
        flags, one_hot(jnp.logical_and(at == rows * me_d + lane_1, lane_1 < rows)), ((1,), (0,))
    )
    col_at = columns * me_s + half * (lax.rem(lane_1, 32) // 16) + lax.rem(lane_1, 16)
    col_flags = dot(
        flags, one_hot(jnp.logical_and(at == col_at, lax.rem(lane_1, 16) < half)), ((1,), (0,))
    )
    spot = lax.broadcasted_iota(jnp.int32, (128, CELLS), 0)
    row_of = lax.broadcasted_iota(jnp.int32, (128, CELLS), 1) // 32
    row_mask = dot(row_flags.astype(BF16), one_hot(spot == row_of), ((1,), (0,)))
    col_mask = jnp.concatenate([col_flags] * (CELLS // 128), axis=1)
    mask = (row_mask * col_mask)[0:1]

    loads[0].wait()
    xt = cells_first(x_ref, 0)
    center = jnp.mean(xt, axis=0, keepdims=True)
    spread = xt - center
    pair_scale = lax.rsqrt(jnp.mean(spread * spread, axis=0, keepdims=True) + EPSILON)
    nt = spread * pair_scale
    normed[...] = nt
    nh = nt.astype(BF16)

    def project(part):
        raw = dot(wp_ref[:, pl.ds(part * hidden, hidden)], nh, ((0,), (0,)))
        return raw

    def edge(part):
        sig = jax.nn.sigmoid(project(part))
        val = project(part + 1)
        proj[part] = sig
        proj[part + 1] = val
        return sig * val * mask

    loads[1].wait()
    leave(LEFT, edge(0))
    leave(RIGHT, edge(2))
    pl.semaphore_wait(barrier, greetings)
    across(RIGHT)
    across(LEFT)

    for load in loads[3:]:
        load.wait()
    gv = jax.nn.sigmoid(dot(wg_ref[...], nh, ((0,), (0,))))
    gate[...] = gv
    ct = cells_first(cot_ref, 1)
    cot[...] = ct
    gh = dot(wo_ref[...], (ct * gv).astype(BF16), ((1,), (0,)))
    ghid[...] = gh - jnp.mean(gh, axis=0, keepdims=True)

    forward(RIGHT, 1)
    forward(LEFT, 0)

    @pl.when(is_owner)
    def _():
        gathered(RIGHT, 1)
        gathered(LEFT, 0)
        for h in range(2):
            multiply(0, 1, ((1,), (1,)), 0, h)
            tiles_back(prod_own, prod_cell, 8 * PRODUCT, h, (0,), True)
        prod_cell[me_s * nz + my_z] = prod_own[me]

    (prod,) = tiles_at_cells(prod_cell, 8 * PRODUCT)
    away = prod - jnp.mean(prod, axis=0, keepdims=True)
    hidden_scale = lax.rsqrt(jnp.mean(away * away, axis=0, keepdims=True) + EPSILON)
    hn = away * hidden_scale
    gh_away = ghid[...]
    second = jnp.mean((gh_away) * hn, axis=0, keepdims=True)
    gprod = hidden_scale * (gh_away - hn * second)
    tiles_to_owners(gprod)

    po = dot(wo_ref[...], hn.astype(BF16), ((0,), (0,)))
    gv = gate[...]
    glogit[...] = (cot[...] * po * gv * (1.0 - gv)).astype(BF16)
    upd_ref[...] = cells_last(gv * po)

    @pl.when(is_owner)
    def _():
        tiles_gathered(2, 0)
        multiply(2, 1, ((1,), (0,)), 0, 0)
        tiles_back(grads_own, grads_cell, 8 * GRADS, 0, (0,), False)
        tiles_gathered(2, 1)
        multiply(2, 0, ((0,), (0,)), 1, 0)
        tiles_back(grads_own, grads_cell, 8 * GRADS, 0, (1,), False)
        multiply(2, 1, ((1,), (0,)), 0, 1)
        multiply(2, 0, ((0,), (0,)), 1, 1)
        tiles_back(grads_own, grads_cell, 8 * GRADS, 1, (0, 1), True)
        grads_cell[me_s * nz + my_z] = grads_own[me]

    base = dot(wg_ref[...], glogit[...], ((1,), (0,)))

    def through(base, part, back):
        masked = back * mask
        sig = proj[part]
        val = proj[part + 1]
        to_sig = (masked * val * sig * (1.0 - sig)).astype(BF16)
        to_val = (masked * sig).astype(BF16)
        base = base + dot(wp_ref[:, pl.ds(part * hidden, hidden)], to_sig, ((1,), (0,)))
        return base + dot(wp_ref[:, pl.ds((part + 1) * hidden, hidden)], to_val, ((1,), (0,)))

    back_left, back_right = tiles_at_cells(grads_cell, 8 * GRADS)
    base = through(base, 0, back_left)
    base = through(base, 2, back_right)

    nt = normed[...]
    first = jnp.mean(base, axis=0, keepdims=True)
    second = jnp.mean(base * nt, axis=0, keepdims=True)
    gpair_ref[...] = cells_last(pair_scale * (base - first - nt * second))

    def sent(ref, count, sem):
        some = ref.at[pl.ds(0, count)]
        push(some, some, sem, {"dap": me_d}).wait_send()

    sent(ch_out.at[LEFT], ns - 1, 8 * LEFT)
    sent(z_out.at[RIGHT], nz - 1, 8 * RIGHT)

    @pl.when(is_owner)
    def _():
        sent(row_out.at[LEFT], nz - 1, 8 * LEFT + 1)
        sent(col_out.at[RIGHT], ns - 1, 8 * RIGHT + 1)
        sent(grad_cell, hidden - 1, 8 * GRAD)
        sent(prod_own, nd * ns - 1, 8 * PRODUCT)
        sent(grads_own, nd * ns - 1, 8 * GRADS)

    @pl.when(jnp.logical_not(is_owner))
    def _():
        sent(row_out.at[LEFT], nz, 8 * LEFT + 1)
        sent(col_out.at[RIGHT], ns, 8 * RIGHT + 1)
        sent(grad_cell, hidden, 8 * GRAD)


def to_hbm(upd, gpair, upd_hbm, gpair_hbm, sem):
    copies = [
        pltpu.make_async_copy(upd, upd_hbm, sem.at[0]),
        pltpu.make_async_copy(gpair, gpair_hbm, sem.at[1]),
    ]
    for copy in copies:
        copy.start()
    for copy in copies:
        copy.wait()


def on_device(nd, ns, pair_rep, residue_mask, w_proj, w_gate, w_out, cotangent):
    hidden, chans = w_out.shape
    vmem = pl.BlockSpec(memory_space=pltpu.VMEM)
    hbm = pl.BlockSpec(memory_space=pltpu.HBM)
    shape = jax.ShapeDtypeStruct(pair_rep.shape, BF16)
    width = ns * 32
    nz = nd // 4
    args = (pair_rep, cotangent, residue_mask[None, :], w_proj, w_gate, w_out)
    args = [pltpu.with_memory_space_constraint(a, pltpu.HBM) for a in args]
    results = pl.pallas_call(
        functools.partial(kernel, nd, ns),
        out_shape=(shape, shape),
        in_specs=[hbm] * 6,
        out_specs=(vmem, vmem),
        scratch_shapes=[pltpu.VMEM(a.shape, a.dtype) for a in args]
        + [
            pltpu.VMEM((2, 16, 32, chans), BF16),
            pltpu.VMEM((8, nd * 16), F32),
            pltpu.VMEM((4, hidden, CELLS), F32),
            pltpu.VMEM((chans, CELLS), F32),
            pltpu.VMEM((chans, CELLS), F32),
            pltpu.VMEM((chans, CELLS), F32),
            pltpu.VMEM((hidden, CELLS), F32),
            pltpu.VMEM((chans, CELLS), BF16),
            pltpu.VMEM((QUADS, 16 * nz, 128), F32),
            pltpu.VMEM((2, ns, nz, CELLS), BF16),
            pltpu.VMEM((2, ns, nz, CELLS), BF16),
            pltpu.VMEM((2, nz, 16, width), BF16),
            pltpu.VMEM((3, nd, 16, width), BF16),
            pltpu.VMEM((2, nz, ns, CELLS), BF16),
            pltpu.VMEM((2, nz, ns, CELLS), BF16),
            pltpu.VMEM((2, ns, nz, CELLS), BF16),
            pltpu.VMEM((2, 4 * ns, nz, CELLS), BF16),
            pltpu.VMEM((ns * nz, 1, QUADS, 128), BF16),
            pltpu.VMEM((nd * ns, 1, QUADS, 128), BF16),
            pltpu.VMEM((ns * nz, QUADS, 128), BF16),
            pltpu.VMEM((nd * ns, QUADS, 128), BF16),
            pltpu.VMEM((ns * nz, 2, QUADS, 128), BF16),
            pltpu.VMEM((nd * ns, 2, QUADS, 128), BF16),
            pltpu.VMEM((2, ns // 4, nd * 16, 128), F32),
            pltpu.VMEM((QUADS * ns * nz, 128), F32),
            pltpu.SemaphoreType.DMA((6,)),
            pltpu.SemaphoreType.DMA((48,)),
            pltpu.SemaphoreType.DMA((48,)),
        ],
        compiler_params=pltpu.CompilerParams(
            collective_id=0, has_side_effects=True, vmem_limit_bytes=50331648
        ),
    )(*args)
    return pl.pallas_call(
        to_hbm,
        out_shape=(shape, shape),
        in_specs=[vmem, vmem],
        out_specs=(hbm, hbm),
        scratch_shapes=[pltpu.SemaphoreType.DMA((2,))],
        compiler_params=pltpu.CompilerParams(vmem_limit_bytes=1024 * 1024),
    )(*results)


def solution(mesh):
    nd, ns = mesh.shape["dap"], mesh.shape["ch"]
    return jax.shard_map(
        functools.partial(on_device, nd, ns),
        mesh=mesh,
        in_specs=(P("dap", "ch", None), P(), P(), P(), P(), P("dap", "ch", None)),
        out_specs=(P("dap", "ch", None), P("dap", "ch", None)),
        check_vma=False,
    )
```

```python
import functools

import jax
import jax.numpy as jnp
from jax import lax
from jax.experimental import pallas as pl
from jax.experimental.pallas import tpu as pltpu
from jax.sharding import PartitionSpec as P

EPSILON = 1e-05
F32 = jnp.float32
BF16 = jnp.bfloat16
CELLS = 512
QUADS = CELLS // 128
LEFT, RIGHT, PRODUCT, GRAD, GRADS = range(5)
ARRIVALS = 40
BY_Z = (RIGHT,)


def ring_order(size):
    return sorted(range(size), key=lambda r: -min(r, size - r))


def ch_peers(me, ch_size):
    ny = ch_size // 2
    steps = [(dy, dx) for dy in range(ny) for dx in range(2) if dy or dx]
    steps.sort(key=lambda p: -(min(p[0], ny - p[0]) + 2 * p[1]))
    y, x = me // 2, lax.rem(me, 2)
    return [2 * lax.rem(y + dy, ny) + lax.rem(x + dx, 2) for dy, dx in steps]


def dot(a, b, contract):
    return lax.dot_general(a, b, (contract, ((), ())), preferred_element_type=F32)


def swap_blocks(rows):
    block = lax.broadcasted_iota(jnp.int32, rows[0].shape, 1) // 32
    odd = lax.rem(block, 2) == 1
    high = block >= 2
    x0, x1, x2, x3 = rows
    z0 = jnp.where(odd, pltpu.roll(x1, 32, 1), x0)
    z1 = jnp.where(odd, x1, pltpu.roll(x0, 96, 1))
    z2 = jnp.where(odd, pltpu.roll(x3, 32, 1), x2)
    z3 = jnp.where(odd, x3, pltpu.roll(x2, 96, 1))
    return (
        jnp.where(high, pltpu.roll(z2, 64, 1), z0),
        jnp.where(high, pltpu.roll(z3, 64, 1), z1),
        jnp.where(high, z2, pltpu.roll(z0, 64, 1)),
        jnp.where(high, z3, pltpu.roll(z1, 64, 1)),
    )


def cells_to_rows(cells, first, count, mid, rows, place):
    group = cells.shape[1]
    for t in range(count // 4):
        for q in range(QUADS):
            lanes = pl.ds(q * 128, 128)
            moved = swap_blocks([cells[first + 4 * t + a, :, lanes].astype(F32) for a in range(4)])
            for b in range(4):
                mid[t, pl.ds(4 * q + b, group, stride=16), :] = moved[b]
    for t in range(count // 4):
        for m in range(group):
            rows[place(m), :, pl.ds(t * 128, 128)] = mid[t, pl.ds(16 * m, 16), :].astype(BF16)


def swap_leading(src, mid, dst):
    na, nb = src.shape[0], src.shape[1]
    for q in range(QUADS):
        lanes = pl.ds(q * 128, 128)
        for a in range(na):
            mid[q, pl.ds(a * nb, nb), :] = src[a, :, lanes].astype(F32)
        for b in range(nb):
            dst[b, :, lanes] = mid[q, pl.ds(b, na, stride=nb), :].astype(BF16)


def kernel(
    nd,
    ns,
    x_hbm,
    cot_hbm,
    mask_hbm,
    wp_hbm,
    wg_hbm,
    wo_hbm,
    upd_ref,
    gpair_ref,
    x_ref,
    cot_ref,
    mask_ref,
    wp_ref,
    wg_ref,
    wo_ref,
    padded,
    live,
    proj,
    normed,
    gate,
    cot,
    ghid,
    glogit,
    mid,
    ch_out,
    ch_in,
    row_out,
    own_in,
    z_out,
    z_in,
    col_out,
    own_cells,
    prod_cell,
    prod_own,
    grad_cell,
    grad_own,
    grads_cell,
    grads_own,
    own_mid,
    flat,
    load_sem,
    send_sem,
    recv_sem,
):
    rows, columns, chans = x_ref.shape
    half = columns // 2
    nz = nd // 4
    hidden = ns * nz
    me_d = lax.axis_index("dap")
    me_s = lax.axis_index("ch")
    my_x, my_z, my_core = me_d // (2 * nz), lax.rem(me_d // 2, nz), lax.rem(me_d, 2)
    is_owner = jnp.logical_and(my_core == 1, my_x == lax.rem(my_z + me_s // 2, 2))

    def at_dap(x, z, core):
        return 2 * nz * x + 2 * z + core

    def owner_of(z, s):
        return at_dap(lax.rem(z + s // 2, 2), z, 1)

    near_ch = ch_peers(me_s, ns)
    z_order = [lax.rem(my_z + r, nz) for r in ring_order(nz)]
    other_x = 1 - my_x
    dap_order = [
        at_dap(x, z, core)
        for z in z_order
        for x in (other_x, my_x)
        for core in (0, 1)
    ][:-1]
    quarters = [(other_x, 0), (other_x, 1), (my_x, 0), (my_x, 1)]

    loads = [
        pltpu.make_async_copy(src, dst, load_sem.at[n])
        for n, (src, dst) in enumerate(
            (
                (x_hbm, x_ref),
                (wp_hbm, wp_ref),
                (mask_hbm, mask_ref),
                (cot_hbm, cot_ref),
                (wg_hbm, wg_ref),
                (wo_hbm, wo_ref),
            )
        )
    ]
    for load in loads:
        load.start()

    barrier = pltpu.get_barrier_semaphore()

    def greet(peer):
        pl.semaphore_signal(
            barrier, inc=1, device_id=peer, device_id_type=pl.DeviceIdType.MESH
        )

    for s in near_ch:
        greet({"ch": s})
    for z in z_order[:-1]:
        greet({"dap": at_dap(my_x, z, my_core)})

    @pl.when(is_owner)
    def _():
        for d in dap_order:
            greet({"dap": d})
        for x, core in quarters:
            for s in near_ch:
                greet({"dap": at_dap(x, my_z, core), "ch": s})
        for x, core in quarters[:-1]:
            greet({"dap": at_dap(x, my_z, core), "ch": me_s})

    @pl.when(jnp.logical_not(is_owner))
    def _():
        for z in z_order:
            greet({"dap": owner_of(z, me_s)})
        for s in near_ch + [me_s]:
            greet({"dap": owner_of(my_z, s), "ch": s})

    greetings = (
        ns - 1 + nz - 1 + jnp.where(is_owner, nd - 1 + 4 * ns - 1, nz + ns)
    )

    def push(src, dst, sem, peer, arrival=None):
        return pltpu.make_async_remote_copy(
            src_ref=src,
            dst_ref=dst,
            send_sem=send_sem.at[sem],
            recv_sem=recv_sem.at[sem if arrival is None else arrival],
            device_id=peer,
            device_id_type=pl.DeviceIdType.MESH,
        )

    def await_slabs(ref, count, sem):
        some = ref.at[pl.ds(0, count)]
        push(some, some, sem, {"dap": me_d}).wait_recv()

    def await_all_but_mine(ref, sem):
        @pl.when(is_owner)
        def _():
            await_slabs(ref, ref.shape[0] - 1, sem)

        @pl.when(jnp.logical_not(is_owner))
        def _():
            await_slabs(ref, ref.shape[0], sem)

    def across_ch(n):
        src, dst, sem = ch_out.at[n], ch_in.at[n], 8 * n
        for s in near_ch:
            push(src.at[s], dst.at[me_s], sem, {"ch": s}).start()
        dst[me_s] = src[me_s]

    def across_z(n):
        src, dst, sem = z_out.at[n], z_in.at[n], 8 * n
        for z in z_order[:-1]:
            push(src.at[z], dst.at[my_z], sem, {"dap": at_dap(my_x, z, my_core)}).start()
        dst[my_z] = src[my_z]

    def rows_to_owners(n, a):
        src, dst, sem = row_out.at[n], own_in.at[a], 8 * n + 1

        def send(z):
            push(src.at[z], dst.at[me_d], sem, {"dap": owner_of(z, me_s)}).start()

        for z in z_order[:-1]:
            send(z)

        @pl.when(is_owner)
        def _():
            dst[me_d] = src[my_z]

        @pl.when(jnp.logical_not(is_owner))
        def _():
            send(my_z)

    def columns_to_owners(n):
        quarter = 2 * my_x + my_core
        slot = quarter * ns + me_s
        sem = 8 * n + 1

        def send(s):
            peer = {"dap": owner_of(my_z, s), "ch": s}
            push(col_out.at[n, s], own_cells.at[n, slot], sem, peer, sem + quarter).start()

        for s in near_ch:
            send(s)

        @pl.when(is_owner)
        def _():
            own_cells[n, slot] = col_out[n, me_s]

        @pl.when(jnp.logical_not(is_owner))
        def _():
            send(me_s)

    def leave(n, value):
        if n in BY_Z:
            for q in range(QUADS):
                lanes = slice(q * 128, q * 128 + 128)
                mid[q, 0:hidden, :] = value[:, lanes]
                for z in range(nz):
                    z_out[n, z, :, lanes] = mid[q, pl.ds(z, ns, stride=nz), :].astype(BF16)
        else:
            ch_out[n] = value.reshape(ns, nz, CELLS).astype(BF16)

    def across(n):
        if n in BY_Z:
            across_z(n)
        else:
            across_ch(n)

    def forward(n, a):
        if n in BY_Z:
            await_slabs(z_in.at[n], nz - 1, 8 * n)
            swap_leading(z_in.at[n], mid, col_out.at[n])
            columns_to_owners(n)
        else:
            await_slabs(ch_in.at[n], ns - 1, 8 * n)
            cells_to_rows(ch_in.at[n], 0, ns, mid, row_out.at[n], lambda m: m)
            rows_to_owners(n, a)

    def gathered(n, a):
        if n not in BY_Z:
            await_slabs(own_in.at[a], nd - 1, 8 * n + 1)
            return

        def arrived(x, core, count):
            quarter = 2 * x + core
            await_slabs(own_cells.at[n], count, 8 * n + 1 + quarter)
            cells_to_rows(
                own_cells.at[n],
                quarter * ns,
                ns,
                mid,
                own_in.at[a],
                lambda z: at_dap(x, z, core),
            )

        arrived(my_x, 1, ns - 1)

        @pl.loop(0, 3)
        def _(r):
            arrived(jnp.where(r == 0, my_x, other_x), lax.rem(r, 2), ns)

    width = ns * 32
    many = nd * 16
    tiles = ns // 4

    hz = nz // 2
    my_half = my_z // hz
    run = 2 * hz

    def multiply(a, b, contract, k, h):
        right = own_in[b].reshape(many, width)
        firsts = [(2 * x + h) * run for x in range(2)]
        if contract[0][0] == 1:
            parts = [own_in[a, pl.ds(f, run)].reshape(16 * run, width) for f in firsts]
        else:
            parts = [own_in[a, :, :, pl.ds(16 * f, 16 * run)].reshape(many, 16 * run) for f in firsts]
        value = dot(jnp.concatenate(parts, axis=1 - contract[0][0]), right, contract)
        for x, f in enumerate(firsts):
            for t in range(tiles):
                own_mid[k, t, pl.ds(16 * f, 16 * run), :] = value[
                    16 * run * x : 16 * run * (x + 1), t * 128 : t * 128 + 128
                ]

    my_tile = me_s // 4
    me = me_d * ns + me_s

    def tile_at(step):
        shift = jnp.where(lax.rem(step, 2) == 1, -((step + 1) // 2), step // 2)
        return lax.rem(my_tile + tiles // 2 + shift, tiles)

    def half_pairs(h):
        return [x * nz + h * hz + z for x in range(2) for z in range(hz)]

    def tiles_back(own, cell, sem, h, kinds, whole):
        mine = me_s * nz + my_z
        turn = jnp.where(my_half == h, 0, hz // 2)
        zs = [h * hz + lax.rem(my_z + r + turn, hz) for r in ring_order(hz)]
        places = [(x, z) for z in zs for x in (other_x, my_x)]

        @pl.loop(0, tiles)
        def _(step):
            t = tile_at(step)
            for k in kinds:
                for p in half_pairs(h):
                    moved = swap_blocks(
                        [own_mid[k, t, pl.ds(32 * p + b, 8, stride=4), :] for b in range(4)]
                    )
                    for a in range(4):
                        line = moved[a].astype(BF16)
                        for core in range(2):
                            own[(2 * p + core) * ns + 4 * t + a, k] = line[4 * core : 4 * core + 4]
            for n, (x, z) in enumerate(places):
                for core in range(2):
                    d = at_dap(x, z, core)
                    for a in range(4):
                        s = 4 * t + a

                        def send(d=d, s=s):
                            src, dst = own.at[d * ns + s], cell.at[mine]
                            if not whole:
                                src, dst = src.at[kinds[0]], dst.at[kinds[0]]
                            push(src, dst, sem, {"dap": d, "ch": s}).start()

                        if n == nz - 1 and core == 1:
                            pl.when(d * ns + s != me)(send)
                        else:
                            send()

    def tiles_at_cells(cell, sem):
        await_all_but_mine(cell, sem)
        found = []
        for k in range(cell.shape[1]):
            for c in range(hidden):
                flat[pl.ds(4 * c, 4), :] = cell[c, k].astype(F32)
            found.append(
                jnp.concatenate(
                    [flat[pl.ds(q, hidden, stride=QUADS), :] for q in range(QUADS)], axis=1
                )
            )
        return found

    def tiles_to_owners(value):
        n = GRAD
        for q in range(QUADS):
            flat[pl.ds(q, hidden, stride=QUADS), :] = value[:, q * 128 : q * 128 + 128]
        for c in range(hidden // 2):
            pair = flat[pl.ds(8 * c, 8), :].astype(BF16)
            grad_cell[2 * c] = pair[0:4]
            grad_cell[2 * c + 1] = pair[4:8]

        ny = ns // 2
        steps = [(dz, dy, dx) for dz in range(nz) for dy in range(ny) for dx in range(2)]
        steps.sort(key=lambda p: -(min(p[0], nz - p[0]) + min(p[1], ny - p[1]) + 2 * p[2]))
        for dz, dy, dx in steps:
            z = lax.rem(my_z + dz, nz)
            s = 2 * lax.rem(me_s // 2 + dy, ny) + lax.rem(me_s + dx, 2)

            def send(z=z, s=s):
                push(
                    grad_cell.at[s * nz + z],
                    grad_own.at[me],
                    8 * n,
                    {"dap": owner_of(z, s), "ch": s},
                    ARRIVALS + 4 * my_half + my_tile,
                ).start()

            if dz or dy or dx:
                send()
            else:
                pl.when(jnp.logical_not(is_owner))(send)

        @pl.when(is_owner)
        def _():
            grad_own[me] = grad_cell[me_s * nz + my_z]

    def tiles_gathered(a, h):
        @pl.loop(0, tiles)
        def _(step):
            t = tile_at(tiles - 1 - step)

            def arrived(count):
                some = grad_own.at[pl.ds(0, count)]
                push(some, some, 8 * GRAD, {"dap": me_d}, ARRIVALS + 4 * h + t).wait_recv()

            mine_too = jnp.logical_and(t == my_tile, my_half == h)
            pl.when(mine_too)(lambda: arrived(2 * nd - 1))
            pl.when(jnp.logical_not(mine_too))(lambda: arrived(2 * nd))
            for p in half_pairs(h):
                got = [
                    jnp.concatenate(
                        [
                            grad_own[(2 * p + core) * ns + 4 * t + e].astype(F32)
                            for core in range(2)
                        ],
                        axis=0,
                    )
                    for e in range(4)
                ]
                for b, rows in enumerate(swap_blocks(got)):
                    own_mid[0, t, pl.ds(32 * p + b, 8, stride=4), :] = rows
            lanes = pl.ds(pl.multiple_of(t * 128, 128), 128)
            for d in [2 * p + core for p in half_pairs(h) for core in range(2)]:
                own_in[a, d, :, lanes] = own_mid[0, t, pl.ds(16 * d, 16), :].astype(BF16)

    lane = lax.broadcasted_iota(jnp.int32, (1, CELLS), 1)
    place = lax.rem(lane, 16)
    used = jnp.logical_and(place < half, lane < rows * 32)
    first_half = lax.rem(lane, 32) < 16

    eye = (
        lax.broadcasted_iota(jnp.int32, (chans, chans), 0)
        == lax.broadcasted_iota(jnp.int32, (chans, chans), 1)
    ).astype(F32).astype(BF16)

    def cells_first(ref, slot):
        padded[slot] = jnp.zeros(padded.shape[1:], BF16)
        padded[slot, 0:rows, 0:columns, :] = ref[...]
        flat = padded[slot].reshape(CELLS, chans)
        turned = dot(eye, flat, ((1,), (1,)))
        spread = jnp.where(first_half, turned, pltpu.roll(turned, 1, 1))
        return jnp.where(used, spread, 0.0)

    def cells_last(turned):
        closed = jnp.where(
            lax.rem(lane, 32) < half, turned, pltpu.roll(turned, CELLS - 1, 1)
        )
        return closed.T.reshape(16, 32, chans)[0:rows, 0:columns, :].astype(BF16)

    residues = mask_ref.shape[1]
    total = nd * 16
    loads[2].wait()
    live[...] = jnp.zeros(live.shape, F32)
    live[:, 0:residues] = jnp.broadcast_to(mask_ref[...].astype(F32), (8, residues))
    flags = live[...].astype(BF16)

    def one_hot(hot):
        return jnp.where(hot, 1.0, 0.0).astype(BF16)

    at = lax.broadcasted_iota(jnp.int32, (total, 128), 0)
    lane_1 = lax.broadcasted_iota(jnp.int32, (total, 128), 1)
    row_flags = dot(
        flags, one_hot(jnp.logical_and(at == rows * me_d + lane_1, lane_1 < rows)), ((1,), (0,))
    )
    col_at = columns * me_s + half * (lax.rem(lane_1, 32) // 16) + lax.rem(lane_1, 16)
    col_flags = dot(
        flags, one_hot(jnp.logical_and(at == col_at, lax.rem(lane_1, 16) < half)), ((1,), (0,))
    )
    spot = lax.broadcasted_iota(jnp.int32, (128, CELLS), 0)
    row_of = lax.broadcasted_iota(jnp.int32, (128, CELLS), 1) // 32
    row_mask = dot(row_flags.astype(BF16), one_hot(spot == row_of), ((1,), (0,)))
    col_mask = jnp.concatenate([col_flags] * (CELLS // 128), axis=1)
    mask = (row_mask * col_mask)[0:1]

    loads[0].wait()
    xt = cells_first(x_ref, 0)
    center = jnp.mean(xt, axis=0, keepdims=True)
    spread = xt - center
    pair_scale = lax.rsqrt(jnp.mean(spread * spread, axis=0, keepdims=True) + EPSILON)
    nt = spread * pair_scale
    normed[...] = nt
    nh = nt.astype(BF16)

    def project(part):
        raw = dot(wp_ref[:, pl.ds(part * hidden, hidden)], nh, ((0,), (0,)))
        return raw

    def edge(part):
        sig = jax.nn.sigmoid(project(part))
        val = project(part + 1)
        proj[part] = sig
        proj[part + 1] = val
        return sig * val * mask

    loads[1].wait()
    leave(LEFT, edge(0))
    leave(RIGHT, edge(2))
    pl.semaphore_wait(barrier, greetings)
    across(RIGHT)
    across(LEFT)

    for load in loads[3:]:
        load.wait()
    gv = jax.nn.sigmoid(dot(wg_ref[...], nh, ((0,), (0,))))
    gate[...] = gv
    ct = cells_first(cot_ref, 1)
    cot[...] = ct
    gh = dot(wo_ref[...], (ct * gv).astype(BF16), ((1,), (0,)))
    ghid[...] = gh - jnp.mean(gh, axis=0, keepdims=True)

    forward(RIGHT, 1)
    forward(LEFT, 0)

    @pl.when(is_owner)
    def _():
        gathered(RIGHT, 1)
        gathered(LEFT, 0)
        for h in range(2):
            multiply(0, 1, ((1,), (1,)), 0, h)
            tiles_back(prod_own, prod_cell, 8 * PRODUCT, h, (0,), True)
        prod_cell[me_s * nz + my_z] = prod_own[me]

    (prod,) = tiles_at_cells(prod_cell, 8 * PRODUCT)
    away = prod - jnp.mean(prod, axis=0, keepdims=True)
    hidden_scale = lax.rsqrt(jnp.mean(away * away, axis=0, keepdims=True) + EPSILON)
    hn = away * hidden_scale
    gh_away = ghid[...]
    second = jnp.mean((gh_away) * hn, axis=0, keepdims=True)
    gprod = hidden_scale * (gh_away - hn * second)
    tiles_to_owners(gprod)

    po = dot(wo_ref[...], hn.astype(BF16), ((0,), (0,)))
    gv = gate[...]
    glogit[...] = (cot[...] * po * gv * (1.0 - gv)).astype(BF16)
    upd_ref[...] = cells_last(gv * po)

    @pl.when(is_owner)
    def _():
        tiles_gathered(2, 0)
        multiply(2, 1, ((1,), (0,)), 0, 0)
        tiles_back(grads_own, grads_cell, 8 * GRADS, 0, (0,), False)
        tiles_gathered(2, 1)
        multiply(2, 0, ((0,), (0,)), 1, 0)
        tiles_back(grads_own, grads_cell, 8 * GRADS, 0, (1,), False)
        multiply(2, 1, ((1,), (0,)), 0, 1)
        multiply(2, 0, ((0,), (0,)), 1, 1)
        tiles_back(grads_own, grads_cell, 8 * GRADS, 1, (0, 1), True)
        grads_cell[me_s * nz + my_z] = grads_own[me]

    base = dot(wg_ref[...], glogit[...], ((1,), (0,)))

    def through(base, part, back):
        masked = back * mask
        sig = proj[part]
        val = proj[part + 1]
        to_sig = (masked * val * sig * (1.0 - sig)).astype(BF16)
        to_val = (masked * sig).astype(BF16)
        base = base + dot(wp_ref[:, pl.ds(part * hidden, hidden)], to_sig, ((1,), (0,)))
        return base + dot(wp_ref[:, pl.ds((part + 1) * hidden, hidden)], to_val, ((1,), (0,)))

    back_left, back_right = tiles_at_cells(grads_cell, 8 * GRADS)
    base = through(base, 0, back_left)
    base = through(base, 2, back_right)

    nt = normed[...]
    first = jnp.mean(base, axis=0, keepdims=True)
    second = jnp.mean(base * nt, axis=0, keepdims=True)
    gpair_ref[...] = cells_last(pair_scale * (base - first - nt * second))

    def sent(ref, count, sem):
        some = ref.at[pl.ds(0, count)]
        push(some, some, sem, {"dap": me_d}).wait_send()

    sent(ch_out.at[LEFT], ns - 1, 8 * LEFT)
    sent(z_out.at[RIGHT], nz - 1, 8 * RIGHT)

    @pl.when(is_owner)
    def _():
        sent(row_out.at[LEFT], nz - 1, 8 * LEFT + 1)
        sent(col_out.at[RIGHT], ns - 1, 8 * RIGHT + 1)
        sent(grad_cell, hidden - 1, 8 * GRAD)
        sent(prod_own, nd * ns - 1, 8 * PRODUCT)
        sent(grads_own, nd * ns - 1, 8 * GRADS)

    @pl.when(jnp.logical_not(is_owner))
    def _():
        sent(row_out.at[LEFT], nz, 8 * LEFT + 1)
        sent(col_out.at[RIGHT], ns, 8 * RIGHT + 1)
        sent(grad_cell, hidden, 8 * GRAD)


def to_hbm(upd, gpair, upd_hbm, gpair_hbm, sem):
    copies = [
        pltpu.make_async_copy(upd, upd_hbm, sem.at[0]),
        pltpu.make_async_copy(gpair, gpair_hbm, sem.at[1]),
    ]
    for copy in copies:
        copy.start()
    for copy in copies:
        copy.wait()


def on_device(nd, ns, pair_rep, residue_mask, w_proj, w_gate, w_out, cotangent):
    hidden, chans = w_out.shape
    vmem = pl.BlockSpec(memory_space=pltpu.VMEM)
    hbm = pl.BlockSpec(memory_space=pltpu.HBM)
    shape = jax.ShapeDtypeStruct(pair_rep.shape, BF16)
    width = ns * 32
    nz = nd // 4
    args = (pair_rep, cotangent, residue_mask[None, :], w_proj, w_gate, w_out)
    args = [pltpu.with_memory_space_constraint(a, pltpu.HBM) for a in args]
    results = pl.pallas_call(
        functools.partial(kernel, nd, ns),
        out_shape=(shape, shape),
        in_specs=[hbm] * 6,
        out_specs=(vmem, vmem),
        scratch_shapes=[pltpu.VMEM(a.shape, a.dtype) for a in args]
        + [
            pltpu.VMEM((2, 16, 32, chans), BF16),
            pltpu.VMEM((8, nd * 16), F32),
            pltpu.VMEM((4, hidden, CELLS), F32),
            pltpu.VMEM((chans, CELLS), F32),
            pltpu.VMEM((chans, CELLS), F32),
            pltpu.VMEM((chans, CELLS), F32),
            pltpu.VMEM((hidden, CELLS), F32),
            pltpu.VMEM((chans, CELLS), BF16),
            pltpu.VMEM((QUADS, 16 * nz, 128), F32),
            pltpu.VMEM((2, ns, nz, CELLS), BF16),
            pltpu.VMEM((2, ns, nz, CELLS), BF16),
            pltpu.VMEM((2, nz, 16, width), BF16),
            pltpu.VMEM((3, nd, 16, width), BF16),
            pltpu.VMEM((2, nz, ns, CELLS), BF16),
            pltpu.VMEM((2, nz, ns, CELLS), BF16),
            pltpu.VMEM((2, ns, nz, CELLS), BF16),
            pltpu.VMEM((2, 4 * ns, nz, CELLS), BF16),
            pltpu.VMEM((ns * nz, 1, QUADS, 128), BF16),
            pltpu.VMEM((nd * ns, 1, QUADS, 128), BF16),
            pltpu.VMEM((ns * nz, QUADS, 128), BF16),
            pltpu.VMEM((nd * ns, QUADS, 128), BF16),
            pltpu.VMEM((ns * nz, 2, QUADS, 128), BF16),
            pltpu.VMEM((nd * ns, 2, QUADS, 128), BF16),
            pltpu.VMEM((2, ns // 4, nd * 16, 128), F32),
            pltpu.VMEM((QUADS * ns * nz, 128), F32),
            pltpu.SemaphoreType.DMA((6,)),
            pltpu.SemaphoreType.DMA((48,)),
            pltpu.SemaphoreType.DMA((48,)),
        ],
        compiler_params=pltpu.CompilerParams(
            collective_id=0, has_side_effects=True, vmem_limit_bytes=50331648
        ),
    )(*args)
    return pl.pallas_call(
        to_hbm,
        out_shape=(shape, shape),
        in_specs=[vmem, vmem],
        out_specs=(hbm, hbm),
        scratch_shapes=[pltpu.SemaphoreType.DMA((2,))],
        compiler_params=pltpu.CompilerParams(vmem_limit_bytes=1024 * 1024),
    )(*results)


def solution(mesh):
    nd, ns = mesh.shape["dap"], mesh.shape["ch"]
    return jax.shard_map(
        functools.partial(on_device, nd, ns),
        mesh=mesh,
        in_specs=(P("dap", "ch", None), P(), P(), P(), P(), P("dap", "ch", None)),
        out_specs=(P("dap", "ch", None), P("dap", "ch", None)),
        check_vma=False,
    )
```
